256 devices in a mesh: gx: 16 (over z, core), gy: 16 (over x, y).
Axes of the slice: x: 4, y: 4, z: 8, core: 2. Of those that a mesh axis runs over, the one named last changes fastest.
Arguments:
- positions: float32 [3, 32, 128, 128], P(None, 'gx', 'gy'), may hold values from 0 to 1
- embed: bfloat16 [32, 128, 128, 256], P('gx', 'gy'), may hold values from -0.75 to 0.75
- counts: int32 [32, 128], P('gx', 'gy'), may hold values from 0 to 128, as said below
- neighbours: int32 [32, 128, 9], P('gx', 'gy'), may hold values from 0 to 40, as said below
- w_one: bfloat16 [256, 256], replicated, may hold values from -0.375 to 0.375
- bias_one: float32 [256], replicated, may hold values from -4 to 4
- w_two: bfloat16 [256, 256], replicated, may hold values from -0.375 to 0.375
- w_out: float32 [256], replicated, may hold values from -0.375 to 0.375
Outputs:
- forces: float32 [3, 32, 128, 128], P(None, 'gx', 'gy')
- energies: float32 [32, 128, 128], P('gx', 'gy')
The draws below stay inside these ranges and needn't reach their ends.
Inputs may be any that keep to these rules, and one draw needn't show every extreme that they name: `counts`: each device's block of 2 x 8 bins has at most 16 non-empty bins, and some devices have exactly 16. The number of non-empty bins of every device's block is a multiple of the size of gy. The blocks of all devices that share a gx index hold together at most 10 times the size of gy non-empty bins, and some such row holds exactly that many. `neighbours`: entry k of a bin at (x, y) of its device's block is 40 or (x + k // 3) * 10 + y + k % 3, the bin offset by (k // 3 - 1, k % 3 - 1) in the block extended by one ghost bin on every side; entry 4 is always present.
All inputs are finite; a program needn't handle non-finite values.
Results may differ from the reference program's by a relative error of at most 0.014.
Values may be sent and summed in bfloat16 or wider, within the bound.
A program may use at most 64 MiB of HBM per device.

```python
import jax
import jax.numpy as jnp
from jax import lax

BX = 2
BY = 8
ATOMS = 128
DESC = 256
HIDDEN_SIZE = 256
NBX = 32
NBY = 128
EXT = 40


def draw_counts(key, part):
    key = jax.random.fold_in(key, 7)
    grid_x = NBX // BX
    grid_y = NBY // BY
    bin_count = BX * BY
    keys = jax.random.split(key, 4)
    film_scores = jax.random.randint(keys[0], (grid_x, grid_y), 0, 1 << 16) * grid_y + jnp.arange(grid_y, dtype=jnp.int32)
    film_rank = jnp.argsort(jnp.argsort(film_scores, axis=-1), axis=-1)
    half_row = grid_y // 2
    film = film_rank < half_row
    sparse_rank = film_rank - half_row
    total_units = bin_count // 8
    base_units = total_units // half_row + (sparse_rank < total_units % half_row).astype(jnp.int32)
    keeping = jax.random.randint(keys[1], (grid_x, grid_y), 0, 2)
    row_index = jnp.arange(grid_x, dtype=jnp.int32)[:, None]
    keeping = jnp.where(row_index == 0, 1, keeping)
    sparse = grid_y * base_units * keeping
    filled = jnp.where(film, bin_count, sparse)
    scores = jax.random.randint(keys[2], (grid_x, grid_y, bin_count), 0, 1 << 16) * bin_count + jnp.arange(bin_count, dtype=jnp.int32)
    standing = jnp.argsort(jnp.argsort(scores, axis=-1), axis=-1)
    live_bins = standing < filled[:, :, None]
    atom_counts = jax.random.randint(keys[3], (grid_x, grid_y, bin_count), ATOMS // 4, ATOMS + 1)
    filled_counts = jnp.where(live_bins, atom_counts, 0)
    return filled_counts.reshape(grid_x, grid_y, BX, BY).transpose(0, 2, 1, 3).reshape(NBX, NBY).astype(jnp.int32)


def draw_neighbours(key, part):
    key = jax.random.fold_in(key, 11)
    keeping = jax.random.randint(key, (NBX, NBY, 9), 0, 4) > 0
    keeping = keeping.at[:, :, 4].set(True)
    row_x = (jnp.arange(NBX, dtype=jnp.int32) % BX)[:, None, None]
    col_y = (jnp.arange(NBY, dtype=jnp.int32) % BY)[None, :, None]
    offset = jnp.arange(9, dtype=jnp.int32)[None, None, :]
    linked = (row_x + offset // 3) * (BY + 2) + col_y + offset % 3
    return jnp.where(keeping, linked, (BX + 2) * (BY + 2)).astype(jnp.int32)


def shard_levels(own_key, dims, cuts, low, high):
    factor_of, own = 1.0, jax.random.fold_in(own_key, 6)
    for dim, blocks in cuts:
        steps = jnp.exp(jax.random.uniform(jax.random.fold_in(own, dim), (blocks,), jnp.float32, low / len(cuts), high / len(cuts)))
        factor_of = factor_of * jnp.repeat(steps, dims[dim] // blocks).reshape([-1 if axis == dim else 1 for axis in range(len(dims))])
    return factor_of


def normal_values(rng, dims, width, most, cuts=(), kind=jnp.bfloat16):
    entries = width * jax.random.normal(rng, dims, jnp.float32)
    if cuts:
        entries = entries * shard_levels(rng, dims, cuts, -0.22, 0.18)
    return jnp.clip(entries, -most, most).astype(kind)


def setup_inputs(seed: int = 0) -> dict:
    key_list = jax.random.split(jax.random.key(seed), 9)
    positions = jnp.clip(1.0 * jax.random.uniform(key_list[0], (3, NBX, NBY, ATOMS), jnp.float32) ** shard_levels(key_list[0], (3, NBX, NBY, ATOMS), ((1, 16), (2, 16)), -0.2, 0.2), 0.0, 1.0)
    embed = normal_values(key_list[1], (NBX, NBY, ATOMS, DESC), 0.125, 0.75, ((0, 16), (1, 16)))
    counts = draw_counts(jax.random.fold_in(key_list[8], 71), 0)
    neighbours = draw_neighbours(jax.random.fold_in(key_list[8], 71), 0)
    w_one = normal_values(key_list[4], (DESC, HIDDEN_SIZE), DESC ** -0.5, 0.375)
    bias_one = normal_values(key_list[5], (HIDDEN_SIZE,), 1.0, 4.0, (), jnp.float32)
    w_two = normal_values(key_list[6], (HIDDEN_SIZE, HIDDEN_SIZE), HIDDEN_SIZE ** -0.5, 0.375)
    w_out = normal_values(key_list[7], (HIDDEN_SIZE,), HIDDEN_SIZE ** -0.5, 0.375, (), jnp.float32)
    return {"positions": positions, "embed": embed, "counts": counts, "neighbours": neighbours, "w_one": w_one, "bias_one": bias_one, "w_two": w_two, "w_out": w_out}


radius = 0.4


def network(features, w_one, bias_one, w_two, w_out):
    flat_rows = features.reshape(-1, features.shape[-1])
    act_one = jnp.tanh(jnp.dot(flat_rows, w_one, preferred_element_type=jnp.float32) + bias_one)
    act_two = jnp.tanh(jnp.dot(act_one.astype(jnp.bfloat16), w_two, preferred_element_type=jnp.float32))
    energy = jnp.sum(act_two * w_out, axis=-1)
    back_two = (w_out * (1.0 - act_two * act_two)).astype(jnp.bfloat16)
    back_one = (jnp.dot(back_two, w_two.T, preferred_element_type=jnp.float32) * (1.0 - act_one * act_one)).astype(jnp.bfloat16)
    gradients = jnp.dot(back_one, w_one.T, preferred_element_type=jnp.float32).astype(jnp.bfloat16)
    return gradients.reshape(features.shape), energy.reshape(features.shape[:-1])


def pair_weights(own_pos, own_mask, remote_pos, remote_mask, shift_x, shift_y):
    delta_x = shift_x[:, None, None] + remote_pos[0][:, None, :] - own_pos[0][:, :, None]
    delta_y = shift_y[:, None, None] + remote_pos[1][:, None, :] - own_pos[1][:, :, None]
    delta_z = remote_pos[2][:, None, :] - own_pos[2][:, :, None]
    square = delta_x * delta_x + delta_y * delta_y + delta_z * delta_z
    weight = jnp.exp(-square / (2.0 * radius * radius)) * own_mask[:, :, None] * remote_mask[:, None, :]
    return weight, delta_x, delta_y, delta_z


def reference(positions, embed, counts, neighbours, w_one, bias_one, w_two, w_out):
    bins_x, bins_y = counts.shape
    per_bin = positions.shape[-1]
    atom_index = jnp.arange(per_bin, dtype=jnp.int32)
    occupied = (atom_index[None, None, :] < counts[:, :, None]).astype(jnp.float32)
    pos_pad = jnp.pad(positions, ((0, 0), (1, 1), (1, 1), (0, 0)), mode="wrap")
    mask_pad = jnp.pad(occupied, ((1, 1), (1, 1), (0, 0)), mode="wrap")
    embed_pad = jnp.pad(embed, ((1, 1), (1, 1), (0, 0), (0, 0)), mode="wrap")
    col_index = jnp.arange(bins_y, dtype=jnp.int32)

    def gather_bin(row_x, neighbour):
        linked = neighbours[row_x, :, neighbour]
        present = linked < EXT
        step_x = jnp.where(present, linked // (BY + 2) - (row_x % BX + 1), 0).astype(jnp.int32)
        step_y = jnp.where(present, linked % (BY + 2) - (col_index % BY + 1), 0).astype(jnp.int32)
        pad_x = row_x + 1 + step_x
        pad_y = col_index + 1 + step_y
        remote_pos = pos_pad[:, pad_x, pad_y]
        remote_mask = mask_pad[pad_x, pad_y] * present[:, None].astype(jnp.float32)
        remote_embed = embed_pad[pad_x, pad_y]
        return remote_pos, remote_mask, remote_embed, step_x.astype(jnp.float32), step_y.astype(jnp.float32), pad_x, pad_y

    def describe(row_x):
        own_pos = positions[:, row_x]
        own_mask = occupied[row_x]
        summed = jnp.zeros((bins_y, per_bin, embed.shape[-1]), jnp.float32)
        for neighbour in range(9):
            remote_pos, remote_mask, remote_embed, shift_x, shift_y, pad_x, pad_y = gather_bin(row_x, neighbour)
            weight, delta_x, delta_y, delta_z = pair_weights(own_pos, own_mask, remote_pos, remote_mask, shift_x, shift_y)
            rounded = lax.optimization_barrier(weight.astype(jnp.bfloat16)).astype(jnp.float32)
            summed = summed + jnp.einsum("bij,bjf->bif", rounded, remote_embed.astype(jnp.float32))
        return summed.astype(jnp.bfloat16)

    features = lax.map(describe, jnp.arange(bins_x, dtype=jnp.int32))

    def evaluate(block):
        return network(block, w_one, bias_one, w_two, w_out)

    gradients, energy = lax.map(evaluate, features)

    def push(ghost_sum, row_x):
        own_pos = positions[:, row_x]
        own_mask = occupied[row_x]
        own_grad = gradients[row_x].astype(jnp.float32)
        own_force = jnp.zeros((3, bins_y, per_bin), jnp.float32)
        for neighbour in range(9):
            remote_pos, remote_mask, remote_embed, shift_x, shift_y, pad_x, pad_y = gather_bin(row_x, neighbour)
            weight, delta_x, delta_y, delta_z = pair_weights(own_pos, own_mask, remote_pos, remote_mask, shift_x, shift_y)
            projected = jnp.einsum("bif,bjf->bij", own_grad, remote_embed.astype(jnp.float32))
            strength = projected * weight / (radius * radius)
            moved = [strength * delta_x, strength * delta_y, strength * delta_z]
            own_force = own_force - jnp.stack([jnp.sum(part, axis=2) for part in moved])
            pushed = jnp.stack([jnp.sum(part, axis=1) for part in moved])
            ghost_sum = ghost_sum.at[:, pad_x, pad_y].add(pushed)
        ghost_sum = ghost_sum.at[:, row_x + 1, col_index + 1].add(own_force)
        return ghost_sum, None

    ghost = jnp.zeros((3, bins_x + 2, bins_y + 2, per_bin), jnp.float32)
    ghost, _ = lax.scan(push, ghost, jnp.arange(bins_x, dtype=jnp.int32))
    middle = ghost[:, 1:bins_x + 1]
    middle = middle.at[:, 0].add(ghost[:, bins_x + 1]).at[:, bins_x - 1].add(ghost[:, 0])
    forces = middle[:, :, 1:bins_y + 1]
    forces = forces.at[:, :, 0].add(middle[:, :, bins_y + 1]).at[:, :, bins_y - 1].add(middle[:, :, 0])
    return forces, energy * occupied
```

```python
import functools

import jax
import jax.numpy as jnp
from jax import lax
from jax.experimental import pallas as pl
from jax.experimental.pallas import tpu as pltpu
from jax.sharding import PartitionSpec as P

MESH = pl.DeviceIdType.MESH
F32 = jnp.float32
BF16 = jnp.bfloat16
radius = 0.4
INV = 1.0 / (radius * radius)
KAPPA = 1.4426950408889634 / (2.0 * radius * radius)
OFF = -30000.0
BX, BY, ATOMS, FEAT, HID = 2, 8, 128, 256, 256
EX, EY = BX + 2, BY + 2
GROUPS = BX * BY // 2
DIRS = ((-1, -1), (-1, 1), (1, -1), (1, 1), (0, -1), (0, 1), (-1, 0), (1, 0))


def rim(step, size):
    return pl.ds(1, 1) if step < 0 else pl.ds(size, 1) if step > 0 else pl.ds(1, size)


def ghost(step, size):
    return pl.ds(0, 1) if step < 0 else pl.ds(size + 1, 1) if step > 0 else pl.ds(1, size)


def split3(value):
    high = value.astype(BF16).astype(F32)
    rest = value - high
    middle = rest.astype(BF16).astype(F32)
    return high, middle, rest - middle


def kernel(
    nx, ny,
    pos_hbm, emb_hbm, cnt, nbr, w1_hbm, b1_hbm, w2_hbm, wo_hbm,
    f_out, e_out,
    emb, emb_t, raw, glob, rows, cols, weight, feat, act, grad, sums, ghost_f, recv_f,
    pos, w1, b1, w2, wo, w1_t, w2_t,
    local_sem, p_send, p_recv, e_send, e_recv, f_send, f_recv,
):
    gx, gy = lax.axis_index("gx"), lax.axis_index("gy")

    def peer(dx, dy):
        return (lax.rem(gx + (dx + nx), nx), lax.rem(gy + (dy + ny), ny))

    barrier = pltpu.get_barrier_semaphore()
    for dx, dy in DIRS:
        pl.semaphore_signal(barrier, inc=1, device_id=peer(dx, dy), device_id_type=MESH)

    loads = [
        pltpu.make_async_copy(pos_hbm, pos, local_sem.at[0]),
        pltpu.make_async_copy(emb_hbm, emb.at[pl.ds(1, BX), pl.ds(1, BY)], local_sem.at[1]),
        pltpu.make_async_copy(w1_hbm, w1, local_sem.at[2]),
        pltpu.make_async_copy(b1_hbm, b1, local_sem.at[3]),
        pltpu.make_async_copy(w2_hbm, w2, local_sem.at[4]),
        pltpu.make_async_copy(wo_hbm, wo, local_sem.at[5]),
    ]
    for load in loads:
        load.start()

    def sends(src, dst, send_sem, recv_sem):
        return [
            pltpu.make_async_remote_copy(
                src_ref=src.at[rim(dx, BX), rim(dy, BY)],
                dst_ref=dst.at[ghost(-dx, BX), ghost(-dy, BY)],
                send_sem=send_sem.at[i],
                recv_sem=recv_sem.at[i],
                device_id=peer(dx, dy),
                device_id_type=MESH,
            )
            for i, (dx, dy) in enumerate(DIRS)
        ]

    p_copies = sends(raw, raw, p_send, p_recv)
    e_copies = sends(emb, emb, e_send, e_recv)
    f_copies = [
        pltpu.make_async_remote_copy(
            src_ref=ghost_f.at[ghost(dx, BX), ghost(dy, BY)],
            dst_ref=recv_f.at[ghost(-dx, BX), ghost(-dy, BY)],
            send_sem=f_send.at[i],
            recv_sem=f_recv.at[i],
            device_id=peer(dx, dy),
            device_id_type=MESH,
        )
        for i, (dx, dy) in enumerate(DIRS)
    ]

    loads[0].wait()
    lane = lax.broadcasted_iota(jnp.int32, (1, ATOMS), 1)
    for x in range(BX):
        for y in range(BY):
            tile = jnp.concatenate(
                [pos[c, x, y : y + 1, :] for c in range(3)]
                + [jnp.where(lane < cnt[x, y], 0.0, OFF).astype(F32)]
                + [jnp.zeros((4, ATOMS), F32)],
                axis=0,
            )
            raw[1 + x, 1 + y] = tile

    pl.semaphore_wait(barrier, len(DIRS))
    for copy in p_copies:
        copy.start()
    loads[1].wait()
    for copy in e_copies:
        copy.start()

    row = lax.broadcasted_iota(jnp.int32, (8, ATOMS), 0)
    mark = lax.broadcasted_iota(jnp.int32, (80, ATOMS), 0)

    def make_rows(ex, ey):
        tile = raw[ex, ey]
        place = tile + jnp.where(row == 0, ex - 1.5, jnp.where(row == 1, ey - 5.0, jnp.where(row == 2, -0.5, 0.0)))
        glob[ex, ey] = place
        square = place * place
        bias = place[3:4] - KAPPA * (square[0:1] + square[1:2] + square[2:3])
        full = jnp.where(row < 3, place, jnp.where(row == 3, bias, jnp.where(row == 4, 1.0, 0.0)))
        high, middle, low = split3(full)
        one_hot = jnp.where(mark == ex * EY + ey, 1.0, 0.0)
        rows[ex, ey] = jnp.concatenate([high, middle, low, high, middle, high, one_hot], axis=0).astype(BF16)
        return place, bias

    def make_cols(x, y, place, bias):
        full = jnp.where(row < 3, (2.0 * KAPPA) * place, jnp.where(row == 3, 1.0, jnp.where(row == 4, bias, 0.0)))
        high, middle, low = split3(full)
        present = mark == nbr[x, y, 0]
        for k in range(1, 9):
            present = jnp.logical_or(present, mark == nbr[x, y, k])
        missing = jnp.where(present, 0.0, OFF)
        stack = jnp.concatenate([high, high, high, middle, middle, low, missing], axis=0)
        cols[x, y] = jnp.transpose(stack).astype(BF16)

    def flip(ex, ey):
        emb_t[ex, ey] = jnp.transpose(emb[ex, ey])

    for x in range(BX):
        for y in range(BY):
            place, bias = make_rows(1 + x, 1 + y)
            make_cols(x, y, place, bias)
    for load in loads[2:]:
        load.wait()
    w1_t[...] = jnp.transpose(w1[...])
    w2_t[...] = jnp.transpose(w2[...])
    for x in range(BX):
        for y in range(BY):
            flip(1 + x, 1 + y)
    sums[...] = jnp.zeros_like(sums)

    for copy in p_copies:
        copy.wait_recv()
    for ey in range(EY):
        make_rows(0, ey)
        make_rows(EX - 1, ey)
    for ex in range(1, EX - 1):
        make_rows(ex, 0)
        make_rows(ex, EY - 1)

    def weights_of(g):
        x, y = g // (BY // 2), 2 * (g % (BY // 2))
        left = jnp.concatenate([cols[x, y], cols[x, y + 1]], axis=0)
        for dr in range(3):
            right = jnp.concatenate([rows[x + dr, y + c] for c in range(4)], axis=1)
            power = jnp.dot(left, right, preferred_element_type=F32)
            weight[g, dr] = jnp.exp2(power).astype(BF16)

    for g in range(GROUPS):
        weights_of(g)

    for copy in e_copies:
        copy.wait_recv()
    for ey in range(EY):
        flip(0, ey)
        flip(EX - 1, ey)
    for ex in range(1, EX - 1):
        flip(ex, 0)
        flip(ex, EY - 1)

    def features_of(g):
        x, y = g // (BY // 2), 2 * (g % (BY // 2))
        total = None
        for dr in range(3):
            block = emb[x + dr, pl.ds(y, 4)].reshape(4 * ATOMS, FEAT)
            part = jnp.dot(weight[g, dr], block, preferred_element_type=F32)
            total = part if total is None else total + part
        feat[g] = total.astype(BF16)

    for g in range(GROUPS):
        features_of(g)

    out_row = wo[...]
    bias_row = b1[...]
    for g in range(GROUPS):
        act[g] = jnp.tanh(jnp.dot(feat[g], w1[...], preferred_element_type=F32) + bias_row)
    for g in range(GROUPS):
        x, y = g // (BY // 2), 2 * (g % (BY // 2))
        two = jnp.tanh(jnp.dot(act[g].astype(BF16), w2[...], preferred_element_type=F32))
        scaled = two * out_row
        halves = scaled[:, :128] + scaled[:, 128:]
        for b in range(2):
            turned = jnp.transpose(halves[b * ATOMS : (b + 1) * ATOMS])
            energy = jnp.sum(turned, axis=0, keepdims=True)
            e_out[x, y + b : y + b + 1, :] = jnp.where(lane < cnt[x, y + b], energy, 0.0)
        feat[g] = (out_row * (1.0 - two * two)).astype(BF16)
    for g in range(GROUPS):
        one = act[g]
        back = jnp.dot(feat[g], w2_t[...], preferred_element_type=F32) * (1.0 - one * one)
        grad[g] = jnp.dot(back.astype(BF16), w1_t[...], preferred_element_type=F32).astype(BF16)

    def forces_of(g):
        x, y = g // (BY // 2), 2 * (g % (BY // 2))
        slope = grad[g]
        own = jnp.concatenate([rows[x + 1, y + 1, 0:16], rows[x + 1, y + 2, 0:16]], axis=1)
        total = None
        for dr in range(3):
            right = jnp.concatenate([emb_t[x + dr, y + c] for c in range(4)], axis=1)
            projected = jnp.dot(slope, right, preferred_element_type=F32)
            strength = projected.astype(BF16) * weight[g, dr]
            other = jnp.concatenate([rows[x + dr, y + c, 0:16] for c in range(4)], axis=1)
            part = lax.dot_general(
                strength, other, (((1,), (1,)), ((), ())), preferred_element_type=F32
            )
            total = part if total is None else total + part
            pushed = jnp.dot(own, strength, preferred_element_type=F32)
            for c in range(4):
                sums[x + dr, y + c] += pushed[:, c * ATOMS : (c + 1) * ATOMS]
        turned = jnp.transpose(total)
        for b in range(2):
            sums[x + 1, y + 1 + b] += turned[:, b * ATOMS : (b + 1) * ATOMS]

    for g in range(GROUPS):
        forces_of(g)

    def force_tile(ex, ey):
        moment = sums[ex, ey, 0:8] + sums[ex, ey, 8:16]
        return (glob[ex, ey] * moment[4:5] - moment) * INV

    for ey in range(EY):
        ghost_f[0, ey] = force_tile(0, ey)
        ghost_f[EX - 1, ey] = force_tile(EX - 1, ey)
    for ex in range(1, EX - 1):
        ghost_f[ex, 0] = force_tile(ex, 0)
        ghost_f[ex, EY - 1] = force_tile(ex, EY - 1)
    for x in range(BX):
        for y in range(BY):
            sums[1 + x, 1 + y, 0:8] = force_tile(1 + x, 1 + y)
    for copy in f_copies:
        copy.start()
    for copy in f_copies:
        copy.wait_recv()
    for x in range(BX):
        outer = 0 if x == 0 else EX - 1
        for y in range(BY):
            tile = sums[1 + x, 1 + y, 0:8] + recv_f[outer, 1 + y]
            if y == 0:
                tile = tile + recv_f[1 + x, 0] + recv_f[outer, 0]
            if y == BY - 1:
                tile = tile + recv_f[1 + x, EY - 1] + recv_f[outer, EY - 1]
            for c in range(3):
                f_out[c, x, y : y + 1, :] = tile[c : c + 1]
    for copies in (p_copies, e_copies, f_copies):
        for copy in copies:
            copy.wait_send()


def solution(mesh):
    nx, ny = mesh.shape["gx"], mesh.shape["gy"]

    def body(positions, embed, counts, neighbours, w_one, bias_one, w_two, w_out):
        hbm = pl.BlockSpec(memory_space=pl.ANY)
        smem = pl.BlockSpec(memory_space=pltpu.SMEM)
        vmem = pl.BlockSpec(memory_space=pltpu.VMEM)
        return pl.pallas_call(
            functools.partial(kernel, nx, ny),
            out_shape=(
                jax.ShapeDtypeStruct((3, BX, BY, ATOMS), F32),
                jax.ShapeDtypeStruct((BX, BY, ATOMS), F32),
            ),
            in_specs=[hbm, hbm, smem, smem, hbm, hbm, hbm, hbm],
            out_specs=(vmem, vmem),
            scratch_shapes=[
                pltpu.VMEM((EX, EY, ATOMS, FEAT), BF16),
                pltpu.VMEM((EX, EY, FEAT, ATOMS), BF16),
                pltpu.VMEM((EX, EY, 8, ATOMS), F32),
                pltpu.VMEM((EX, EY, 8, ATOMS), F32),
                pltpu.VMEM((EX, EY, 128, ATOMS), BF16),
                pltpu.VMEM((BX, BY, ATOMS, 128), BF16),
                pltpu.VMEM((GROUPS, 3, 2 * ATOMS, 4 * ATOMS), BF16),
                pltpu.VMEM((GROUPS, 2 * ATOMS, FEAT), BF16),
                pltpu.VMEM((GROUPS, 2 * ATOMS, HID), F32),
                pltpu.VMEM((GROUPS, 2 * ATOMS, FEAT), BF16),
                pltpu.VMEM((EX, EY, 16, ATOMS), F32),
                pltpu.VMEM((EX, EY, 8, ATOMS), F32),
                pltpu.VMEM((EX, EY, 8, ATOMS), F32),
                pltpu.VMEM((3, BX, BY, ATOMS), F32),
                pltpu.VMEM((FEAT, HID), BF16),
                pltpu.VMEM((1, HID), F32),
                pltpu.VMEM((HID, HID), BF16),
                pltpu.VMEM((1, HID), F32),
                pltpu.VMEM((HID, FEAT), BF16),
                pltpu.VMEM((HID, HID), BF16),
                pltpu.SemaphoreType.DMA((6,)),
                pltpu.SemaphoreType.DMA((8,)),
                pltpu.SemaphoreType.DMA((8,)),
                pltpu.SemaphoreType.DMA((8,)),
                pltpu.SemaphoreType.DMA((8,)),
                pltpu.SemaphoreType.DMA((8,)),
                pltpu.SemaphoreType.DMA((8,)),
            ],
            compiler_params=pltpu.CompilerParams(
                collective_id=0, has_side_effects=True, vmem_limit_bytes=60 * 1024 * 1024
            ),
        )(positions, embed, counts, neighbours, w_one, bias_one[None], w_two, w_out[None])

    in_specs = (
        P(None, "gx", "gy", None),
        P("gx", "gy", None, None),
        P("gx", "gy"),
        P("gx", "gy", None),
        P(),
        P(),
        P(),
        P(),
    )
    out_specs = (P(None, "gx", "gy", None), P("gx", "gy", None))
    return jax.shard_map(body, mesh=mesh, in_specs=in_specs, out_specs=out_specs, check_vma=False)
```

```python
import functools

import jax
import jax.numpy as jnp
from jax import lax
from jax.experimental import pallas as pl
from jax.experimental.pallas import tpu as pltpu
from jax.sharding import PartitionSpec as P

MESH = pl.DeviceIdType.MESH
F32 = jnp.float32
BF16 = jnp.bfloat16
radius = 0.4
INV = 1.0 / (radius * radius)
KAPPA = 1.4426950408889634 / (2.0 * radius * radius)
OFF = -30000.0
BX, BY, ATOMS, FEAT, HID = 2, 8, 128, 256, 256
EX, EY = BX + 2, BY + 2
GROUPS = BX * BY // 2
DIRS = ((-1, 0), (-1, -1), (-1, 1), (0, -1), (0, 1), (1, 0), (1, -1), (1, 1))


def rim(step, size):
    return pl.ds(1, 1) if step < 0 else pl.ds(size, 1) if step > 0 else pl.ds(1, size)


def ghost(step, size):
    return pl.ds(0, 1) if step < 0 else pl.ds(size + 1, 1) if step > 0 else pl.ds(1, size)


def split3(value):
    high = value.astype(BF16).astype(F32)
    rest = value - high
    middle = rest.astype(BF16).astype(F32)
    return high, middle, rest - middle


def kernel(
    nx, ny,
    pos_hbm, emb_hbm, cnt, nbr, w1_hbm, b1_hbm, w2_hbm, wo_hbm,
    f_out, e_out,
    emb, emb_t, raw, glob, rows, cols, weight, feat, act, grad, sums, ghost_f, recv_f,
    pos, w1, b1, w2, wo, w1_t, w2_t,
    local_sem, p_send, p_recv, e_send, e_recv, f_send, f_recv,
):
    gx, gy = lax.axis_index("gx"), lax.axis_index("gy")
    odd = lax.rem(gx, 2)
    sign = 1 - 2 * odd
    turn = sign.astype(F32)

    def peer(side, dy):
        return (lax.rem(gx + side * sign + nx, nx), lax.rem(gy + (dy + ny), ny))

    def home(x):
        return x + odd * (1 - 2 * x)

    barrier = pltpu.get_barrier_semaphore()
    for side, dy in DIRS:
        pl.semaphore_signal(barrier, inc=1, device_id=peer(side, dy), device_id_type=MESH)

    loads = [
        pltpu.make_async_copy(pos_hbm, pos, local_sem.at[0]),
        pltpu.make_async_copy(emb_hbm.at[home(0)], emb.at[1, pl.ds(1, BY)], local_sem.at[1]),
        pltpu.make_async_copy(emb_hbm.at[home(1)], emb.at[2, pl.ds(1, BY)], local_sem.at[6]),
        pltpu.make_async_copy(w1_hbm, w1, local_sem.at[2]),
        pltpu.make_async_copy(b1_hbm, b1, local_sem.at[3]),
        pltpu.make_async_copy(w2_hbm, w2, local_sem.at[4]),
        pltpu.make_async_copy(wo_hbm, wo, local_sem.at[5]),
    ]
    for load in loads:
        load.start()

    def send(src, dst, send_sem, recv_sem, i, target):
        return pltpu.make_async_remote_copy(
            src_ref=src, dst_ref=dst, send_sem=send_sem.at[i], recv_sem=recv_sem.at[i],
            device_id=target, device_id_type=MESH,
        )

    p_copies = [
        send(raw.at[rim(side, BX), rim(dy, BY)], raw.at[ghost(side, BX), ghost(-dy, BY)],
             p_send, p_recv, i, peer(side, dy))
        for i, (side, dy) in enumerate(DIRS)
    ]
    f_copies = [
        send(ghost_f.at[ghost(side, BX), ghost(dy, BY)], recv_f.at[ghost(side, BX), ghost(-dy, BY)],
             f_send, f_recv, i, peer(side, dy))
        for i, (side, dy) in enumerate(DIRS)
    ]
    lo, hi, mid, all_y, both = pl.ds(1, 1), pl.ds(BY, 1), pl.ds(2, BY - 2), pl.ds(1, BY), pl.ds(1, BX)
    west, east = pl.ds(0, 1), pl.ds(BY + 1, 1)
    routes = (
        (both, lo, both, east, 0, -1),
        (both, hi, both, west, 0, 1),
        (pl.ds(1, 1), lo, pl.ds(0, 1), lo, -1, 0),
        (pl.ds(1, 1), hi, pl.ds(0, 1), hi, -1, 0),
        (pl.ds(1, 1), mid, pl.ds(0, 1), mid, -1, 0),
        (pl.ds(2, 1), all_y, pl.ds(3, 1), all_y, 1, 0),
        (pl.ds(3, 1), lo, pl.ds(3, 1), east, 0, -1),
        (pl.ds(3, 1), hi, pl.ds(3, 1), west, 0, 1),
        (pl.ds(0, 1), lo, pl.ds(0, 1), east, 0, -1),
        (pl.ds(0, 1), hi, pl.ds(0, 1), west, 0, 1),
    )
    e_copies = [
        send(emb.at[sx, sy], emb.at[tx, ty], e_send, e_recv, i, peer(side, dy))
        for i, (sx, sy, tx, ty, side, dy) in enumerate(routes)
    ]
    cols_in, far_edges, far_mid, near_in = e_copies[0:2], e_copies[2:4], e_copies[4:5], e_copies[5:6]
    near_relay, far_relay = e_copies[6:8], e_copies[8:10]

    def start(copies):
        for copy in copies:
            copy.start()

    def arrive(copies):
        for copy in copies:
            copy.wait_recv()

    loads[0].wait()
    lane = lax.broadcasted_iota(jnp.int32, (1, ATOMS), 1)
    for x in range(BX):
        for y in range(BY):
            tile = jnp.concatenate(
                [pos[c, home(x), y : y + 1, :] for c in range(3)]
                + [jnp.where(lane < cnt[home(x), y], 0.0, OFF).astype(F32)]
                + [jnp.zeros((4, ATOMS), F32)],
                axis=0,
            )
            raw[1 + x, 1 + y] = tile

    pl.semaphore_wait(barrier, len(DIRS))
    start(p_copies)
    loads[1].wait()
    start(far_edges + far_mid)
    loads[2].wait()
    start(near_in + cols_in)

    row = lax.broadcasted_iota(jnp.int32, (8, ATOMS), 0)
    mark = lax.broadcasted_iota(jnp.int32, (80, ATOMS), 0)

    def make_rows(ex, ey):
        tile = raw[ex, ey]
        place = tile + jnp.where(
            row == 0, turn * (ex - 1.5), jnp.where(row == 1, ey - 5.0, jnp.where(row == 2, -0.5, 0.0))
        )
        glob[ex, ey] = place
        square = place * place
        bias = place[3:4] - KAPPA * (square[0:1] + square[1:2] + square[2:3])
        full = jnp.where(row < 3, place, jnp.where(row == 3, bias, jnp.where(row == 4, 1.0, 0.0)))
        high, middle, low = split3(full)
        one_hot = jnp.where(mark == (ex + odd * (EX - 1 - 2 * ex)) * EY + ey, 1.0, 0.0)
        rows[ex, ey] = jnp.concatenate([high, middle, low, high, middle, high, one_hot], axis=0).astype(BF16)
        return place, bias

    def make_cols(x, y, place, bias):
        full = jnp.where(row < 3, (2.0 * KAPPA) * place, jnp.where(row == 3, 1.0, jnp.where(row == 4, bias, 0.0)))
        high, middle, low = split3(full)
        present = mark == nbr[home(x), y, 0]
        for k in range(1, 9):
            present = jnp.logical_or(present, mark == nbr[home(x), y, k])
        missing = jnp.where(present, 0.0, OFF)
        stack = jnp.concatenate([high, high, high, middle, middle, low, missing], axis=0)
        cols[x, y] = jnp.transpose(stack).astype(BF16)

    def flip(ex, ey):
        emb_t[ex, ey] = jnp.transpose(emb[ex, ey])

    for x in range(BX):
        for y in range(BY):
            place, bias = make_rows(1 + x, 1 + y)
            make_cols(x, y, place, bias)
    for load in loads[3:]:
        load.wait()
    w1_t[...] = jnp.transpose(w1[...])
    w2_t[...] = jnp.transpose(w2[...])
    for x in range(BX):
        for y in range(BY):
            flip(1 + x, 1 + y)
    sums[...] = jnp.zeros_like(sums)

    arrive(near_in)
    start(near_relay)
    arrive(p_copies)
    for ey in range(EY):
        make_rows(EX - 1, ey)
        make_rows(0, ey)
    for ex in range(1, EX - 1):
        make_rows(ex, 0)
        make_rows(ex, EY - 1)

    def spot(g):
        return g // (BY // 2), 2 * (g % (BY // 2))

    def weights_of(g):
        x, y = spot(g)
        left = jnp.concatenate([cols[x, y], cols[x, y + 1]], axis=0)
        for dr in range(3):
            right = jnp.concatenate([rows[x + dr, y + c] for c in range(4)], axis=1)
            power = jnp.dot(left, right, preferred_element_type=F32)
            weight[g, dr] = jnp.exp2(power).astype(BF16)

    def features_of(g):
        x, y = spot(g)
        total = None
        for dr in range(3):
            block = emb[x + dr, pl.ds(y, 4)].reshape(4 * ATOMS, FEAT)
            part = jnp.dot(weight[g, dr], block, preferred_element_type=F32)
            total = part if total is None else total + part
        feat[g] = total.astype(BF16)

    out_row = wo[...]
    bias_row = b1[...]

    def network(groups):
        for g in groups:
            act[g] = jnp.tanh(jnp.dot(feat[g], w1[...], preferred_element_type=F32) + bias_row)
        for g in groups:
            x, y = spot(g)
            two = jnp.tanh(jnp.dot(act[g].astype(BF16), w2[...], preferred_element_type=F32))
            scaled = two * out_row
            halves = scaled[:, :128] + scaled[:, 128:]
            for b in range(2):
                turned = jnp.transpose(halves[b * ATOMS : (b + 1) * ATOMS])
                energy = jnp.sum(turned, axis=0, keepdims=True)
                e_out[home(x), y + b : y + b + 1, :] = jnp.where(lane < cnt[home(x), y + b], energy, 0.0)
            feat[g] = (out_row * (1.0 - two * two)).astype(BF16)
        for g in groups:
            one = act[g]
            back = jnp.dot(feat[g], w2_t[...], preferred_element_type=F32) * (1.0 - one * one)
            grad[g] = back.astype(BF16)
        for g in groups:
            grad[g] = jnp.dot(grad[g], w1_t[...], preferred_element_type=F32).astype(BF16)

    def forces_of(g, steps):
        x, y = spot(g)
        slope = grad[g]
        own = jnp.concatenate([rows[x + 1, y + 1, 0:16], rows[x + 1, y + 2, 0:16]], axis=1)
        total = None
        for dr in steps:
            right = jnp.concatenate([emb_t[x + dr, y + c] for c in range(4)], axis=1)
            projected = jnp.dot(slope, right, preferred_element_type=F32)
            strength = projected.astype(BF16) * weight[g, dr]
            other = jnp.concatenate([rows[x + dr, y + c, 0:16] for c in range(4)], axis=1)
            part = lax.dot_general(
                strength, other, (((1,), (1,)), ((), ())), preferred_element_type=F32
            )
            total = part if total is None else total + part
            pushed = jnp.dot(own, strength, preferred_element_type=F32)
            for c in range(4):
                sums[x + dr, y + c] += pushed[:, c * ATOMS : (c + 1) * ATOMS]
        turned = jnp.transpose(total)
        for b in range(2):
            sums[x + 1, y + 1 + b] += turned[:, b * ATOMS : (b + 1) * ATOMS]

    def force_tile(ex, ey):
        moment = sums[ex, ey, 0:8] + sums[ex, ey, 8:16]
        return (glob[ex, ey] * moment[4:5] - moment) * INV

    far, near = range(GROUPS // 2), range(GROUPS // 2, GROUPS)
    for g in near:
        weights_of(g)
    arrive(far_edges)
    start(far_relay)
    for g in far:
        weights_of(g)

    arrive(cols_in + near_relay)
    for ey in range(EY):
        flip(EX - 1, ey)
    for ex in range(1, EX - 1):
        flip(ex, 0)
        flip(ex, EY - 1)
    for g in near:
        features_of(g)
    network(near)
    for g in near:
        forces_of(g, (2, 0, 1))
    for ey in range(EY):
        ghost_f[EX - 1, ey] = force_tile(EX - 1, ey)
    start(f_copies[5:8])

    arrive(far_mid + far_relay)
    for ey in range(EY):
        flip(0, ey)
    for g in far:
        features_of(g)
    network(far)
    for g in far:
        forces_of(g, (0,))
    for ey in range(EY):
        ghost_f[0, ey] = force_tile(0, ey)
    start(f_copies[0:3])
    forces_of(0, (1, 2))
    forces_of(3, (1, 2))
    for ex in range(1, EX - 1):
        ghost_f[ex, 0] = force_tile(ex, 0)
        ghost_f[ex, EY - 1] = force_tile(ex, EY - 1)
    start(f_copies[3:5])
    forces_of(1, (1, 2))
    forces_of(2, (1, 2))
    for x in range(BX):
        for y in range(BY):
            sums[1 + x, 1 + y, 0:8] = force_tile(1 + x, 1 + y)
    arrive(f_copies)
    for x in range(BX):
        outer = 0 if x == 0 else EX - 1
        for y in range(BY):
            tile = sums[1 + x, 1 + y, 0:8] + recv_f[outer, 1 + y]
            if y == 0:
                tile = tile + recv_f[1 + x, 0] + recv_f[outer, 0]
            if y == BY - 1:
                tile = tile + recv_f[1 + x, EY - 1] + recv_f[outer, EY - 1]
            for c in range(3):
                f_out[c, home(x), y : y + 1, :] = tile[c : c + 1]
    for copies in (p_copies, e_copies, f_copies):
        for copy in copies:
            copy.wait_send()


def solution(mesh):
    nx, ny = mesh.shape["gx"], mesh.shape["gy"]

    def body(positions, embed, counts, neighbours, w_one, bias_one, w_two, w_out):
        hbm = pl.BlockSpec(memory_space=pl.ANY)
        smem = pl.BlockSpec(memory_space=pltpu.SMEM)
        vmem = pl.BlockSpec(memory_space=pltpu.VMEM)
        return pl.pallas_call(
            functools.partial(kernel, nx, ny),
            out_shape=(
                jax.ShapeDtypeStruct((3, BX, BY, ATOMS), F32),
                jax.ShapeDtypeStruct((BX, BY, ATOMS), F32),
            ),
            in_specs=[hbm, hbm, smem, smem, hbm, hbm, hbm, hbm],
            out_specs=(vmem, vmem),
            scratch_shapes=[
                pltpu.VMEM((EX, EY, ATOMS, FEAT), BF16),
                pltpu.VMEM((EX, EY, FEAT, ATOMS), BF16),
                pltpu.VMEM((EX, EY, 8, ATOMS), F32),
                pltpu.VMEM((EX, EY, 8, ATOMS), F32),
                pltpu.VMEM((EX, EY, 128, ATOMS), BF16),
                pltpu.VMEM((BX, BY, ATOMS, 128), BF16),
                pltpu.VMEM((GROUPS, 3, 2 * ATOMS, 4 * ATOMS), BF16),
                pltpu.VMEM((GROUPS, 2 * ATOMS, FEAT), BF16),
                pltpu.VMEM((GROUPS, 2 * ATOMS, HID), F32),
                pltpu.VMEM((GROUPS, 2 * ATOMS, FEAT), BF16),
                pltpu.VMEM((EX, EY, 16, ATOMS), F32),
                pltpu.VMEM((EX, EY, 8, ATOMS), F32),
                pltpu.VMEM((EX, EY, 8, ATOMS), F32),
                pltpu.VMEM((3, BX, BY, ATOMS), F32),
                pltpu.VMEM((FEAT, HID), BF16),
                pltpu.VMEM((1, HID), F32),
                pltpu.VMEM((HID, HID), BF16),
                pltpu.VMEM((1, HID), F32),
                pltpu.VMEM((HID, FEAT), BF16),
                pltpu.VMEM((HID, HID), BF16),
                pltpu.SemaphoreType.DMA((7,)),
                pltpu.SemaphoreType.DMA((8,)),
                pltpu.SemaphoreType.DMA((8,)),
                pltpu.SemaphoreType.DMA((10,)),
                pltpu.SemaphoreType.DMA((10,)),
                pltpu.SemaphoreType.DMA((8,)),
                pltpu.SemaphoreType.DMA((8,)),
            ],
            compiler_params=pltpu.CompilerParams(
                collective_id=0, has_side_effects=True, vmem_limit_bytes=60 * 1024 * 1024
            ),
        )(positions, embed, counts, neighbours, w_one, bias_one[None], w_two, w_out[None])

    in_specs = (
        P(None, "gx", "gy", None),
        P("gx", "gy", None, None),
        P("gx", "gy"),
        P("gx", "gy", None),
        P(),
        P(),
        P(),
        P(),
    )
    out_specs = (P(None, "gx", "gy", None), P("gx", "gy", None))
    return jax.shard_map(body, mesh=mesh, in_specs=in_specs, out_specs=out_specs, check_vma=False)
```

```python
import functools

import jax
import jax.numpy as jnp
from jax import lax
from jax.experimental import pallas as pl
from jax.experimental.pallas import tpu as pltpu
from jax.sharding import PartitionSpec as P

MESH = pl.DeviceIdType.MESH
F32 = jnp.float32
BF16 = jnp.bfloat16
radius = 0.4
INV = 1.0 / (radius * radius)
KAPPA = 1.4426950408889634 / (2.0 * radius * radius)
OFF = -30000.0
BX, BY, ATOMS, FEAT, HID = 2, 8, 128, 256, 256
EX, EY = BX + 2, BY + 2
GROUPS = BX * BY // 2
DIRS = ((-1, 0), (-1, -1), (-1, 1), (0, -1), (0, 1), (1, 0), (1, -1), (1, 1))


def rim(step, size):
    return pl.ds(1, 1) if step < 0 else pl.ds(size, 1) if step > 0 else pl.ds(1, size)


def ghost(step, size):
    return pl.ds(0, 1) if step < 0 else pl.ds(size + 1, 1) if step > 0 else pl.ds(1, size)


def split3(value):
    high = value.astype(BF16).astype(F32)
    rest = value - high
    middle = rest.astype(BF16).astype(F32)
    return high, middle, rest - middle


def kernel(
    nx, ny,
    pos_hbm, emb_hbm, cnt_hbm, nbr_hbm, w1_hbm, b1_hbm, w2_hbm, wo_hbm,
    out,
    emb, emb_t, raw, glob, rows, cols, w_mid, w_side, feat, act, grad, sums, ghost_f, recv_f,
    pos, cnt, nbr, w1, b1, w2, wo, w1_t, w2_t,
    local_sem, p_send, p_recv, e_send, e_recv, f_send, f_recv,
):
    gx, gy = lax.axis_index("gx"), lax.axis_index("gy")
    odd = lax.rem(gx, 2)
    sign = 1 - 2 * odd
    turn = sign.astype(F32)

    def peer(side, dy):
        return (lax.rem(gx + side * sign + nx, nx), lax.rem(gy + (dy + ny), ny))

    def home(x):
        return x + odd * (1 - 2 * x)

    barrier = pltpu.get_barrier_semaphore()
    for side, dy in DIRS:
        pl.semaphore_signal(barrier, inc=1, device_id=peer(side, dy), device_id_type=MESH)

    loads = [
        pltpu.make_async_copy(pos_hbm, pos, local_sem.at[0]),
        pltpu.make_async_copy(cnt_hbm, cnt, local_sem.at[7]),
        pltpu.make_async_copy(emb_hbm.at[home(0)], emb.at[1, pl.ds(1, BY)], local_sem.at[1]),
        pltpu.make_async_copy(emb_hbm.at[home(1)], emb.at[2, pl.ds(1, BY)], local_sem.at[6]),
        pltpu.make_async_copy(w1_hbm, w1, local_sem.at[2]),
        pltpu.make_async_copy(b1_hbm, b1, local_sem.at[3]),
        pltpu.make_async_copy(w2_hbm, w2, local_sem.at[4]),
        pltpu.make_async_copy(wo_hbm, wo, local_sem.at[5]),
        pltpu.make_async_copy(nbr_hbm, nbr, local_sem.at[8]),
    ]
    for load in loads:
        load.start()

    def send(src, dst, send_sem, recv_sem, i, target):
        return pltpu.make_async_remote_copy(
            src_ref=src, dst_ref=dst, send_sem=send_sem.at[i], recv_sem=recv_sem.at[i],
            device_id=target, device_id_type=MESH,
        )

    p_copies = [
        send(raw.at[rim(side, BX), rim(dy, BY)], raw.at[ghost(side, BX), ghost(-dy, BY)],
             p_send, p_recv, i, peer(side, dy))
        for i, (side, dy) in enumerate(DIRS)
    ]
    f_copies = [
        send(ghost_f.at[ghost(side, BX), ghost(dy, BY)], recv_f.at[ghost(side, BX), ghost(-dy, BY)],
             f_send, f_recv, i, peer(side, dy))
        for i, (side, dy) in enumerate(DIRS)
    ]
    lo, hi, mid, all_y, both = pl.ds(1, 1), pl.ds(BY, 1), pl.ds(2, BY - 2), pl.ds(1, BY), pl.ds(1, BX)
    west, east = pl.ds(0, 1), pl.ds(BY + 1, 1)
    routes = (
        (both, lo, both, east, 0, -1),
        (both, hi, both, west, 0, 1),
        (pl.ds(1, 1), lo, pl.ds(0, 1), lo, -1, 0),
        (pl.ds(1, 1), hi, pl.ds(0, 1), hi, -1, 0),
        (pl.ds(1, 1), mid, pl.ds(0, 1), mid, -1, 0),
        (pl.ds(2, 1), all_y, pl.ds(3, 1), all_y, 1, 0),
        (pl.ds(2, 1), west, pl.ds(3, 1), west, 1, 0),
        (pl.ds(2, 1), east, pl.ds(3, 1), east, 1, 0),
        (pl.ds(0, 1), lo, pl.ds(0, 1), east, 0, -1),
        (pl.ds(0, 1), hi, pl.ds(0, 1), west, 0, 1),
    )
    e_copies = [
        send(emb.at[sx, sy], emb.at[tx, ty], e_send, e_recv, i, peer(side, dy))
        for i, (sx, sy, tx, ty, side, dy) in enumerate(routes)
    ]
    cols_in, far_edges, far_mid, near_in = e_copies[0:2], e_copies[2:4], e_copies[4:5], e_copies[5:6]
    near_relay, far_relay = e_copies[6:8], e_copies[8:10]

    def start(copies):
        for copy in copies:
            copy.start()

    def arrive(copies):
        for copy in copies:
            copy.wait_recv()

    loads[0].wait()
    loads[1].wait()
    lane = lax.broadcasted_iota(jnp.int32, (1, ATOMS), 1)
    for x in range(BX):
        for y in range(BY):
            tile = jnp.concatenate(
                [pos[c, home(x), y : y + 1, :] for c in range(3)]
                + [jnp.where(lane < cnt[home(x), y], 0.0, OFF).astype(F32)]
                + [jnp.zeros((4, ATOMS), F32)],
                axis=0,
            )
            raw[1 + x, 1 + y] = tile

    pl.semaphore_wait(barrier, len(DIRS))
    start(p_copies)
    loads[2].wait()
    start(far_edges + far_mid)
    loads[3].wait()
    start(near_in + cols_in)

    row = lax.broadcasted_iota(jnp.int32, (8, ATOMS), 0)
    mark = lax.broadcasted_iota(jnp.int32, (80, ATOMS), 0)

    def make_rows(ex, ey):
        tile = raw[ex, ey]
        place = tile + jnp.where(
            row == 0, turn * (ex - 1.5), jnp.where(row == 1, ey - 5.0, jnp.where(row == 2, -0.5, 0.0))
        )
        glob[ex, ey] = place
        square = place * place
        bias = place[3:4] - KAPPA * (square[0:1] + square[1:2] + square[2:3])
        full = jnp.where(row < 3, place, jnp.where(row == 3, bias, jnp.where(row == 4, 1.0, 0.0)))
        high, middle, low = split3(full)
        one_hot = jnp.where(mark == (ex + odd * (EX - 1 - 2 * ex)) * EY + ey, 1.0, 0.0)
        rows[ex, ey] = jnp.concatenate([high, middle, low, high, middle, high, one_hot], axis=0).astype(BF16)
        return place, bias

    def make_cols(x, y, place, bias):
        full = jnp.where(row < 3, (2.0 * KAPPA) * place, jnp.where(row == 3, 1.0, jnp.where(row == 4, bias, 0.0)))
        high, middle, low = split3(full)
        present = mark == nbr[home(x), y, 0]
        for k in range(1, 9):
            present = jnp.logical_or(present, mark == nbr[home(x), y, k])
        missing = jnp.where(present, 0.0, OFF)
        stack = jnp.concatenate([high, high, high, middle, middle, low, missing], axis=0)
        cols[x, y] = jnp.transpose(stack).astype(BF16)

    def flip(ex, ey):
        emb_t[ex, ey] = jnp.transpose(emb[ex, ey])

    loads[8].wait()
    def spot(g):
        return g // (BY // 2), 2 * (g % (BY // 2))

    def row_block(x, y, steps, count, height=128):
        return jnp.concatenate([rows[x + dr, y + c, 0:height] for dr in steps for c in range(count)], axis=1)

    def middle_weights(g, steps):
        x, y = spot(g)
        left = jnp.concatenate([cols[x, y], cols[x, y + 1]], axis=0)
        for dr in steps:
            power = jnp.dot(left, row_block(x, y + 1, (dr,), 2), preferred_element_type=F32)
            w_mid[g, dr] = jnp.exp2(power).astype(BF16)

    def side_weights(g):
        x, y = spot(g)
        for b in range(2):
            power = jnp.dot(cols[x, y + b], row_block(x, y + 3 * b, (0, 1, 2), 1), preferred_element_type=F32)
            w_side[g, b] = jnp.exp2(power).astype(BF16)

    def middle_part(g, dr):
        x, y = spot(g)
        block = emb[x + dr, y + 1 : y + 3].reshape(2 * ATOMS, FEAT)
        return jnp.dot(w_mid[g, dr], block, preferred_element_type=F32)

    def own_steps(g):
        return (1, 2) if g < GROUPS // 2 else (0, 1)

    def ghost_step(g):
        return 0 if g < GROUPS // 2 else 2

    def features_of(g):
        x, y = spot(g)
        total = act[g] + middle_part(g, ghost_step(g))
        for b in range(2):
            block = emb[x : x + 3, y + 3 * b].reshape(3 * ATOMS, FEAT)
            part = jnp.dot(w_side[g, b], block, preferred_element_type=F32)
            half = slice(b * ATOMS, (b + 1) * ATOMS)
            feat[g, half] = (total[half] + part).astype(BF16)

    for x in range(BX):
        for y in range(BY):
            place, bias = make_rows(1 + x, 1 + y)
            make_cols(x, y, place, bias)
    for load in loads[4:8]:
        load.wait()
    w1_t[...] = jnp.transpose(w1[...])
    w2_t[...] = jnp.transpose(w2[...])
    for x in range(BX):
        for y in range(BY):
            flip(1 + x, 1 + y)
    sums[...] = jnp.zeros_like(sums)

    for g in range(GROUPS):
        middle_weights(g, own_steps(g))
    for g in range(GROUPS):
        first, second = own_steps(g)
        act[g] = middle_part(g, first) + middle_part(g, second)

    out_row = wo[...]
    bias_row = b1[...]

    def network(groups):
        for g in groups:
            act[g] = jnp.tanh(jnp.dot(feat[g], w1[...], preferred_element_type=F32) + bias_row)
        for g in groups:
            x, y = spot(g)
            two = jnp.tanh(jnp.dot(act[g].astype(BF16), w2[...], preferred_element_type=F32))
            scaled = two * out_row
            halves = scaled[:, :128] + scaled[:, 128:]
            for b in range(2):
                turned = jnp.transpose(halves[b * ATOMS : (b + 1) * ATOMS])
                energy = jnp.sum(turned, axis=0, keepdims=True)
                out[3 * BX + home(x), y + b : y + b + 1, :] = jnp.where(lane < cnt[home(x), y + b], energy, 0.0)
            feat[g] = (out_row * (1.0 - two * two)).astype(BF16)
        for g in groups:
            one = act[g]
            back = jnp.dot(feat[g], w2_t[...], preferred_element_type=F32) * (1.0 - one * one)
            grad[g] = back.astype(BF16)
        for g in groups:
            grad[g] = jnp.dot(grad[g], w1_t[...], preferred_element_type=F32).astype(BF16)

    def ghost_units(g):
        _, y = spot(g)
        units = [(g, 0, 2, (ghost_step(g),), 1, 2)]
        units += [(g, b, 1, (ghost_step(g),), 3 * b, 1) for b in range(2)]
        return units + [(g, b, 1, own_steps(g), 3 * b, 1) for b in range(2) if y + 3 * b in (0, EY - 1)]

    def inner_units(g):
        _, y = spot(g)
        units = [(g, 0, 2, (dr,), 1, 2) for dr in own_steps(g)]
        return units + [(g, b, 1, own_steps(g), 3 * b, 1) for b in range(2) if y + 3 * b not in (0, EY - 1)]

    def project(unit):
        g, first, slots, steps, col, count = unit
        x, y = spot(g)
        right = jnp.concatenate([emb_t[x + dr, y + col + c] for dr in steps for c in range(count)], axis=1)
        slope = grad[g, first * ATOMS : (first + slots) * ATOMS]
        return jnp.dot(slope, right, preferred_element_type=F32)

    def strengthen(unit):
        g, first, slots, steps, col, count = unit
        projected = project(unit).astype(BF16)
        if slots == 2:
            w_mid[g, steps[0]] = projected * w_mid[g, steps[0]]
        else:
            part = slice(steps[0] * ATOMS, (steps[-1] + 1) * ATOMS)
            w_side[g, first, :, part] = projected * w_side[g, first, :, part]

    def spread(unit):
        g, first, slots, steps, col, count = unit
        x, y = spot(g)
        if slots == 2:
            strength = w_mid[g, steps[0]]
        else:
            strength = w_side[g, first, :, steps[0] * ATOMS : (steps[-1] + 1) * ATOMS]
        other = row_block(x, y + col, steps, count, 16)
        part = lax.dot_general(strength, other, (((1,), (1,)), ((), ())), preferred_element_type=F32)
        own = row_block(x, y + 1 + first, (1,), slots, 16)
        pushed = jnp.dot(own, strength, preferred_element_type=F32)
        spots = [(x + dr, y + col + c) for dr in steps for c in range(count)]
        for i, (ex, ey) in enumerate(spots):
            sums[ex, ey] += pushed[:, i * ATOMS : (i + 1) * ATOMS]
        return part

    def forces_of(units):
        for unit in units:
            strengthen(unit)
        gathered = {}
        for unit in units:
            part = spread(unit)
            g, first, slots = unit[:3]
            for b in range(slots):
                piece = part[b * ATOMS : (b + 1) * ATOMS]
                key = (g, first + b)
                gathered[key] = piece if key not in gathered else gathered[key] + piece
        for (g, b), total in gathered.items():
            x, y = spot(g)
            sums[x + 1, y + 1 + b] += jnp.transpose(total)

    def force_tile(ex, ey):
        moment = sums[ex, ey, 0:8] + sums[ex, ey, 8:16]
        return (glob[ex, ey] * moment[4:5] - moment) * INV

    far, near = range(GROUPS // 2), range(GROUPS // 2, GROUPS)
    arrive(p_copies[3:8])
    for ey in range(EY):
        make_rows(EX - 1, ey)
    for ex in range(1, EX - 1):
        make_rows(ex, 0)
        make_rows(ex, EY - 1)
    for g in near:
        middle_weights(g, (2,))
        side_weights(g)
    arrive(p_copies[0:3])
    for ey in range(EY):
        make_rows(0, ey)
    arrive(far_edges)
    start(far_relay)
    for g in far:
        middle_weights(g, (0,))
        side_weights(g)
    arrive(cols_in)
    start(near_relay)
    arrive(near_in)
    for ey in range(1, EY - 1):
        flip(EX - 1, ey)
    for ex in range(1, EX - 1):
        flip(ex, 0)
        flip(ex, EY - 1)
    arrive(near_relay)
    flip(EX - 1, 0)
    flip(EX - 1, EY - 1)
    for g in near:
        features_of(g)
    network(near)
    forces_of([unit for g in near for unit in ghost_units(g)])
    for ey in range(EY):
        ghost_f[EX - 1, ey] = force_tile(EX - 1, ey)
    start(f_copies[5:8])

    arrive(far_mid + far_relay)
    for ey in range(EY):
        flip(0, ey)
    for g in far:
        features_of(g)
    network(far)
    forces_of([unit for g in far for unit in ghost_units(g)])
    for ey in range(EY):
        ghost_f[0, ey] = force_tile(0, ey)
    for ex in range(1, EX - 1):
        ghost_f[ex, 0] = force_tile(ex, 0)
        ghost_f[ex, EY - 1] = force_tile(ex, EY - 1)
    start(f_copies[0:5])
    forces_of([unit for g in near for unit in inner_units(g)])
    forces_of([unit for g in far for unit in inner_units(g)])
    for x in range(BX):
        for y in range(BY):
            sums[1 + x, 1 + y, 0:8] = force_tile(1 + x, 1 + y)
    arrive(f_copies)
    for x in range(BX):
        outer = 0 if x == 0 else EX - 1
        for y in range(BY):
            tile = sums[1 + x, 1 + y, 0:8] + recv_f[outer, 1 + y]
            if y == 0:
                tile = tile + recv_f[1 + x, 0] + recv_f[outer, 0]
            if y == BY - 1:
                tile = tile + recv_f[1 + x, EY - 1] + recv_f[outer, EY - 1]
            for c in range(3):
                out[c * BX + home(x), y : y + 1, :] = tile[c : c + 1]
    for copies in (p_copies, e_copies, f_copies):
        for copy in copies:
            copy.wait_send()


def unpack(packed, forces, energies):
    forces[...] = packed[0 : 3 * BX]
    energies[...] = packed[3 * BX :]


def solution(mesh):
    nx, ny = mesh.shape["gx"], mesh.shape["gy"]

    def body(positions, embed, counts, neighbours, w_one, bias_one, w_two, w_out):
        hbm = pl.BlockSpec(memory_space=pl.ANY)
        vmem = pl.BlockSpec(memory_space=pltpu.VMEM)
        packed = pl.pallas_call(
            functools.partial(kernel, nx, ny),
            out_shape=jax.ShapeDtypeStruct((4 * BX, BY, ATOMS), F32),
            in_specs=[hbm] * 8,
            out_specs=vmem,
            scratch_shapes=[
                pltpu.VMEM((EX, EY, ATOMS, FEAT), BF16),
                pltpu.VMEM((EX, EY, FEAT, ATOMS), BF16),
                pltpu.VMEM((EX, EY, 8, ATOMS), F32),
                pltpu.VMEM((EX, EY, 8, ATOMS), F32),
                pltpu.VMEM((EX, EY, 128, ATOMS), BF16),
                pltpu.VMEM((BX, BY, ATOMS, 128), BF16),
                pltpu.VMEM((GROUPS, 3, 2 * ATOMS, 2 * ATOMS), BF16),
                pltpu.VMEM((GROUPS, 2, ATOMS, 3 * ATOMS), BF16),
                pltpu.VMEM((GROUPS, 2 * ATOMS, FEAT), BF16),
                pltpu.VMEM((GROUPS, 2 * ATOMS, HID), F32),
                pltpu.VMEM((GROUPS, 2 * ATOMS, FEAT), BF16),
                pltpu.VMEM((EX, EY, 16, ATOMS), F32),
                pltpu.VMEM((EX, EY, 8, ATOMS), F32),
                pltpu.VMEM((EX, EY, 8, ATOMS), F32),
                pltpu.VMEM((3, BX, BY, ATOMS), F32),
                pltpu.SMEM((BX, BY), jnp.int32),
                pltpu.SMEM((BX, BY, 9), jnp.int32),
                pltpu.VMEM((FEAT, HID), BF16),
                pltpu.VMEM((1, HID), F32),
                pltpu.VMEM((HID, HID), BF16),
                pltpu.VMEM((1, HID), F32),
                pltpu.VMEM((HID, FEAT), BF16),
                pltpu.VMEM((HID, HID), BF16),
                pltpu.SemaphoreType.DMA((9,)),
                pltpu.SemaphoreType.DMA((8,)),
                pltpu.SemaphoreType.DMA((8,)),
                pltpu.SemaphoreType.DMA((10,)),
                pltpu.SemaphoreType.DMA((10,)),
                pltpu.SemaphoreType.DMA((8,)),
                pltpu.SemaphoreType.DMA((8,)),
            ],
            compiler_params=pltpu.CompilerParams(
                collective_id=0, has_side_effects=True, vmem_limit_bytes=60 * 1024 * 1024
            ),
        )(positions, embed, counts, neighbours, w_one, bias_one[None], w_two, w_out[None])
        forces, energies = pl.pallas_call(
            unpack,
            out_shape=(
                jax.ShapeDtypeStruct((3 * BX, BY, ATOMS), F32),
                jax.ShapeDtypeStruct((BX, BY, ATOMS), F32),
            ),
            in_specs=[vmem],
            out_specs=(vmem, vmem),
        )(packed)
        return forces.reshape(3, BX, BY, ATOMS), energies

    in_specs = (
        P(None, "gx", "gy", None),
        P("gx", "gy", None, None),
        P("gx", "gy"),
        P("gx", "gy", None),
        P(),
        P(),
        P(),
        P(),
    )
    out_specs = (P(None, "gx", "gy", None), P("gx", "gy", None))
    return jax.shard_map(body, mesh=mesh, in_specs=in_specs, out_specs=out_specs, check_vma=False)
```

```python
import functools

import jax
import jax.numpy as jnp
from jax import lax
from jax.experimental import pallas as pl
from jax.experimental.pallas import tpu as pltpu
from jax.sharding import PartitionSpec as P

MESH = pl.DeviceIdType.MESH
F32 = jnp.float32
BF16 = jnp.bfloat16
radius = 0.4
INV = 1.0 / (radius * radius)
KAPPA = 1.4426950408889634 / (2.0 * radius * radius)
OFF = -30000.0
BX, BY, ATOMS, FEAT, HID = 2, 8, 128, 256, 256
EX, EY = BX + 2, BY + 2
GROUPS = BX * BY // 2
DIRS = ((-1, 0), (-1, -1), (-1, 1), (0, -1), (0, 1), (1, 0), (1, -1), (1, 1))


def rim(step, size):
    return pl.ds(1, 1) if step < 0 else pl.ds(size, 1) if step > 0 else pl.ds(1, size)


def ghost(step, size):
    return pl.ds(0, 1) if step < 0 else pl.ds(size + 1, 1) if step > 0 else pl.ds(1, size)


def split3(value):
    high = value.astype(BF16).astype(F32)
    rest = value - high
    middle = rest.astype(BF16).astype(F32)
    return high, middle, rest - middle


def kernel(
    nx, ny,
    pos_hbm, emb_hbm, cnt_hbm, nbr_hbm, w1_hbm, b1_hbm, w2_hbm, wo_hbm,
    out,
    emb, emb_t, raw, glob, rows, cols, w_mid, w_side, feat, act, grad, sums, ghost_f, recv_f,
    pos, cnt, nbr, w1, b1, w2, wo, w1_t, w2_t,
    local_sem, p_send, p_recv, e_send, e_recv, f_send, f_recv,
):
    gx, gy = lax.axis_index("gx"), lax.axis_index("gy")
    odd = lax.rem(gx, 2)
    sign = 1 - 2 * odd
    turn = sign.astype(F32)

    def peer(side, dy):
        return (lax.rem(gx + side * sign + nx, nx), lax.rem(gy + (dy + ny), ny))

    def home(x):
        return x + odd * (1 - 2 * x)

    barrier = pltpu.get_barrier_semaphore()
    for side, dy in DIRS:
        pl.semaphore_signal(barrier, inc=1, device_id=peer(side, dy), device_id_type=MESH)

    loads = [
        pltpu.make_async_copy(pos_hbm, pos, local_sem.at[0]),
        pltpu.make_async_copy(cnt_hbm, cnt, local_sem.at[7]),
        pltpu.make_async_copy(emb_hbm.at[home(0)], emb.at[1, pl.ds(1, BY)], local_sem.at[1]),
        pltpu.make_async_copy(emb_hbm.at[home(1)], emb.at[2, pl.ds(1, BY)], local_sem.at[6]),
        pltpu.make_async_copy(w1_hbm, w1, local_sem.at[2]),
        pltpu.make_async_copy(b1_hbm, b1, local_sem.at[3]),
        pltpu.make_async_copy(w2_hbm, w2, local_sem.at[4]),
        pltpu.make_async_copy(wo_hbm, wo, local_sem.at[5]),
        pltpu.make_async_copy(nbr_hbm, nbr, local_sem.at[8]),
    ]
    for load in loads:
        load.start()

    def send(src, dst, send_sem, recv_sem, i, target):
        return pltpu.make_async_remote_copy(
            src_ref=src, dst_ref=dst, send_sem=send_sem.at[i], recv_sem=recv_sem.at[i],
            device_id=target, device_id_type=MESH,
        )

    p_copies = [
        send(raw.at[rim(side, BX), rim(dy, BY)], raw.at[ghost(side, BX), ghost(-dy, BY)],
             p_send, p_recv, i, peer(side, dy))
        for i, (side, dy) in enumerate(DIRS)
    ]
    f_copies = [
        send(ghost_f.at[ghost(side, BX), ghost(dy, BY)], recv_f.at[ghost(side, BX), ghost(-dy, BY)],
             f_send, f_recv, i, peer(side, dy))
        for i, (side, dy) in enumerate(DIRS)
    ]
    lo, hi, all_y = pl.ds(1, 1), pl.ds(BY, 1), pl.ds(1, BY)
    west, east = pl.ds(0, 1), pl.ds(BY + 1, 1)
    r0, r1, r2, r3 = (pl.ds(i, 1) for i in range(EX))
    routes = (
        (r2, lo, r2, east, 0, -1),
        (r2, hi, r2, west, 0, 1),
        (r1, lo, r1, east, 0, -1),
        (r1, hi, r1, west, 0, 1),
        (r1, lo, r0, lo, -1, 0),
        (r1, hi, r0, hi, -1, 0),
        (r1, pl.ds(2, 2), r0, pl.ds(2, 2), -1, 0),
        (r1, pl.ds(BY - 2, 2), r0, pl.ds(BY - 2, 2), -1, 0),
        (r1, pl.ds(4, BY - 6), r0, pl.ds(4, BY - 6), -1, 0),
        (r2, all_y, r3, all_y, 1, 0),
        (r2, west, r3, west, 1, 0),
        (r2, east, r3, east, 1, 0),
        (r0, lo, r0, east, 0, -1),
        (r0, hi, r0, west, 0, 1),
    )
    e_copies = [
        send(emb.at[sx, sy], emb.at[tx, ty], e_send, e_recv, i, peer(side, dy))
        for i, (sx, sy, tx, ty, side, dy) in enumerate(routes)
    ]
    near_cols, far_cols, far_edges, far_outer, far_inner, near_in = (
        e_copies[i:j] for i, j in ((0, 2), (2, 4), (4, 6), (6, 8), (8, 9), (9, 10))
    )
    near_relay, far_relay = e_copies[10:12], e_copies[12:14]

    def start(copies):
        for copy in copies:
            copy.start()

    def arrive(copies):
        for copy in copies:
            copy.wait_recv()

    loads[0].wait()
    loads[1].wait()
    lane = lax.broadcasted_iota(jnp.int32, (1, ATOMS), 1)
    for x in range(BX):
        for y in range(BY):
            tile = jnp.concatenate(
                [pos[c, home(x), y : y + 1, :] for c in range(3)]
                + [jnp.where(lane < cnt[home(x), y], 0.0, OFF).astype(F32)]
                + [jnp.zeros((4, ATOMS), F32)],
                axis=0,
            )
            raw[1 + x, 1 + y] = tile

    pl.semaphore_wait(barrier, len(DIRS))
    start(p_copies)
    loads[2].wait()
    loads[3].wait()
    start(near_cols + far_edges + near_in + far_cols + far_outer + far_inner)

    row = lax.broadcasted_iota(jnp.int32, (8, ATOMS), 0)
    mark = lax.broadcasted_iota(jnp.int32, (80, ATOMS), 0)

    def make_rows(ex, ey):
        tile = raw[ex, ey]
        place = tile + jnp.where(
            row == 0, turn * (ex - 1.5), jnp.where(row == 1, ey - 5.0, jnp.where(row == 2, -0.5, 0.0))
        )
        glob[ex, ey] = place
        square = place * place
        bias = place[3:4] - KAPPA * (square[0:1] + square[1:2] + square[2:3])
        full = jnp.where(row < 3, place, jnp.where(row == 3, bias, jnp.where(row == 4, 1.0, 0.0)))
        high, middle, low = split3(full)
        one_hot = jnp.where(mark == (ex + odd * (EX - 1 - 2 * ex)) * EY + ey, 1.0, 0.0)
        rows[ex, ey] = jnp.concatenate([high, middle, low, high, middle, high, one_hot], axis=0).astype(BF16)
        return place, bias

    def make_cols(x, y, place, bias):
        full = jnp.where(row < 3, (2.0 * KAPPA) * place, jnp.where(row == 3, 1.0, jnp.where(row == 4, bias, 0.0)))
        high, middle, low = split3(full)
        present = mark == nbr[home(x), y, 0]
        for k in range(1, 9):
            present = jnp.logical_or(present, mark == nbr[home(x), y, k])
        missing = jnp.where(present, 0.0, OFF)
        stack = jnp.concatenate([high, high, high, middle, middle, low, missing], axis=0)
        cols[x, y] = jnp.transpose(stack).astype(BF16)

    def flip(ex, ey):
        emb_t[ex, ey] = jnp.transpose(emb[ex, ey])

    loads[8].wait()
    def spot(g):
        return g // (BY // 2), 2 * (g % (BY // 2))

    def row_block(x, y, steps, count, height=128):
        return jnp.concatenate([rows[x + dr, y + c, 0:height] for dr in steps for c in range(count)], axis=1)

    def middle_weights(g, steps):
        x, y = spot(g)
        left = jnp.concatenate([cols[x, y], cols[x, y + 1]], axis=0)
        for dr in steps:
            power = jnp.dot(left, row_block(x, y + 1, (dr,), 2), preferred_element_type=F32)
            w_mid[g, dr] = jnp.exp2(power).astype(BF16)

    def inner_sides(g):
        _, y = spot(g)
        return [b for b in range(2) if y + 3 * b not in (0, EY - 1)]

    def side_weights(g, b, steps):
        x, y = spot(g)
        power = jnp.dot(cols[x, y + b], row_block(x, y + 3 * b, steps, 1), preferred_element_type=F32)
        w_side[g, b, :, steps[0] * ATOMS : (steps[-1] + 1) * ATOMS] = jnp.exp2(power).astype(BF16)

    def late_sides(g):
        for b in range(2):
            side_weights(g, b, (ghost_step(g),) if b in inner_sides(g) else (0, 1, 2))

    def side_part(g, b, steps):
        x, y = spot(g)
        block = emb[x + steps[0] : x + steps[-1] + 1, y + 3 * b].reshape(len(steps) * ATOMS, FEAT)
        share = w_side[g, b, :, steps[0] * ATOMS : (steps[-1] + 1) * ATOMS]
        return jnp.dot(share, block, preferred_element_type=F32)

    def middle_part(g, dr):
        x, y = spot(g)
        block = emb[x + dr, y + 1 : y + 3].reshape(2 * ATOMS, FEAT)
        return jnp.dot(w_mid[g, dr], block, preferred_element_type=F32)

    def own_steps(g):
        return (1, 2) if g < GROUPS // 2 else (0, 1)

    def ghost_step(g):
        return 0 if g < GROUPS // 2 else 2

    def features_of(g):
        total = act[g] + middle_part(g, ghost_step(g))
        for b in range(2):
            part = side_part(g, b, (ghost_step(g),) if b in inner_sides(g) else (0, 1, 2))
            half = slice(b * ATOMS, (b + 1) * ATOMS)
            feat[g, half] = (total[half] + part).astype(BF16)

    for x in range(BX):
        for y in range(BY):
            place, bias = make_rows(1 + x, 1 + y)
            make_cols(x, y, place, bias)
    for load in loads[4:8]:
        load.wait()
    w1_t[...] = jnp.transpose(w1[...])
    w2_t[...] = jnp.transpose(w2[...])
    for x in range(BX):
        for y in range(BY):
            flip(1 + x, 1 + y)
    sums[...] = jnp.zeros_like(sums)

    for g in range(GROUPS):
        middle_weights(g, own_steps(g))
        for b in inner_sides(g):
            side_weights(g, b, own_steps(g))
    for g in range(GROUPS):
        first, second = own_steps(g)
        total = middle_part(g, first) + middle_part(g, second)
        for b in range(2):
            half = slice(b * ATOMS, (b + 1) * ATOMS)
            inner = b in inner_sides(g)
            act[g, half] = total[half] + side_part(g, b, own_steps(g)) if inner else total[half]

    out_row = wo[...]
    bias_row = b1[...]

    def network(groups):
        for g in groups:
            act[g] = jnp.tanh(jnp.dot(feat[g], w1[...], preferred_element_type=F32) + bias_row)
        for g in groups:
            x, y = spot(g)
            two = jnp.tanh(jnp.dot(act[g].astype(BF16), w2[...], preferred_element_type=F32))
            scaled = two * out_row
            halves = scaled[:, :128] + scaled[:, 128:]
            for b in range(2):
                turned = jnp.transpose(halves[b * ATOMS : (b + 1) * ATOMS])
                energy = jnp.sum(turned, axis=0, keepdims=True)
                out[3 * BX + home(x), y + b : y + b + 1, :] = jnp.where(lane < cnt[home(x), y + b], energy, 0.0)
            feat[g] = (out_row * (1.0 - two * two)).astype(BF16)
        for g in groups:
            one = act[g]
            back = jnp.dot(feat[g], w2_t[...], preferred_element_type=F32) * (1.0 - one * one)
            grad[g] = back.astype(BF16)
        for g in groups:
            grad[g] = jnp.dot(grad[g], w1_t[...], preferred_element_type=F32).astype(BF16)

    def ghost_units(g):
        _, y = spot(g)
        units = [(g, 0, 2, (ghost_step(g),), 1, 2)]
        units += [(g, b, 1, (ghost_step(g),), 3 * b, 1) for b in range(2)]
        return units + [(g, b, 1, own_steps(g), 3 * b, 1) for b in range(2) if y + 3 * b in (0, EY - 1)]

    def inner_units(g):
        _, y = spot(g)
        units = [(g, 0, 2, (dr,), 1, 2) for dr in own_steps(g)]
        return units + [(g, b, 1, own_steps(g), 3 * b, 1) for b in range(2) if y + 3 * b not in (0, EY - 1)]

    def project(unit):
        g, first, slots, steps, col, count = unit
        x, y = spot(g)
        right = jnp.concatenate([emb_t[x + dr, y + col + c] for dr in steps for c in range(count)], axis=1)
        slope = grad[g, first * ATOMS : (first + slots) * ATOMS]
        return jnp.dot(slope, right, preferred_element_type=F32)

    def strengthen(unit):
        g, first, slots, steps, col, count = unit
        projected = project(unit).astype(BF16)
        if slots == 2:
            w_mid[g, steps[0]] = projected * w_mid[g, steps[0]]
        else:
            part = slice(steps[0] * ATOMS, (steps[-1] + 1) * ATOMS)
            w_side[g, first, :, part] = projected * w_side[g, first, :, part]

    def spread(unit):
        g, first, slots, steps, col, count = unit
        x, y = spot(g)
        if slots == 2:
            strength = w_mid[g, steps[0]]
        else:
            strength = w_side[g, first, :, steps[0] * ATOMS : (steps[-1] + 1) * ATOMS]
        other = row_block(x, y + col, steps, count, 16)
        part = lax.dot_general(strength, other, (((1,), (1,)), ((), ())), preferred_element_type=F32)
        own = row_block(x, y + 1 + first, (1,), slots, 16)
        pushed = jnp.dot(own, strength, preferred_element_type=F32)
        spots = [(x + dr, y + col + c) for dr in steps for c in range(count)]
        for i, (ex, ey) in enumerate(spots):
            sums[ex, ey] += pushed[:, i * ATOMS : (i + 1) * ATOMS]
        return part

    def forces_of(units):
        for unit in units:
            strengthen(unit)
        gathered = {}
        for unit in units:
            part = spread(unit)
            g, first, slots = unit[:3]
            for b in range(slots):
                piece = part[b * ATOMS : (b + 1) * ATOMS]
                key = (g, first + b)
                gathered[key] = piece if key not in gathered else gathered[key] + piece
        for (g, b), total in gathered.items():
            x, y = spot(g)
            sums[x + 1, y + 1 + b] += jnp.transpose(total)

    def force_tile(ex, ey):
        moment = sums[ex, ey, 0:8] + sums[ex, ey, 8:16]
        return (glob[ex, ey] * moment[4:5] - moment) * INV

    far, near = range(GROUPS // 2), range(GROUPS // 2, GROUPS)
    arrive(p_copies[3:8])
    for ey in range(EY):
        make_rows(EX - 1, ey)
    for ex in range(1, EX - 1):
        make_rows(ex, 0)
        make_rows(ex, EY - 1)
    for g in near:
        middle_weights(g, (2,))
        late_sides(g)
    arrive(near_cols)
    start(near_relay)
    arrive(p_copies[0:3])
    for ey in range(EY):
        make_rows(0, ey)
    arrive(far_edges)
    start(far_relay)
    arrive(near_in)
    for ey in range(1, EY - 1):
        flip(EX - 1, ey)
    inside, outside = (5, 6), (4, 7)
    for g in inside:
        features_of(g)
    network(inside)
    for g in far:
        middle_weights(g, (0,))
        late_sides(g)
    arrive(far_cols + near_relay)
    for ex in range(1, EX - 1):
        flip(ex, 0)
        flip(ex, EY - 1)
    flip(EX - 1, 0)
    flip(EX - 1, EY - 1)
    for g in outside:
        features_of(g)
    network(outside)
    forces_of([unit for g in inside + outside for unit in ghost_units(g)])
    for ey in range(EY):
        ghost_f[EX - 1, ey] = force_tile(EX - 1, ey)
    start(f_copies[5:8])

    arrive(far_outer + far_relay)
    for ey in (0, 1, 2, 3, 6, 7, 8, 9):
        flip(0, ey)
    for g in (0, 3):
        features_of(g)
    network((0, 3))
    forces_of([unit for g in (0, 3) for unit in ghost_units(g)])
    for ey in (0, EY - 1):
        for ex in range(EX - 1):
            ghost_f[ex, ey] = force_tile(ex, ey)
    start(f_copies[1:5])
    arrive(far_inner)
    for ey in (4, 5):
        flip(0, ey)
    for g in (1, 2):
        features_of(g)
    network((1, 2))
    forces_of([unit for g in (1, 2) for unit in ghost_units(g)])
    for ey in range(1, EY - 1):
        ghost_f[0, ey] = force_tile(0, ey)
    start(f_copies[0:1])
    forces_of([unit for g in near for unit in inner_units(g)])
    forces_of([unit for g in far for unit in inner_units(g)])
    for x in range(BX):
        for y in range(BY):
            sums[1 + x, 1 + y, 0:8] = force_tile(1 + x, 1 + y)
    arrive(f_copies)
    for x in range(BX):
        outer = 0 if x == 0 else EX - 1
        for y in range(BY):
            tile = sums[1 + x, 1 + y, 0:8] + recv_f[outer, 1 + y]
            if y == 0:
                tile = tile + recv_f[1 + x, 0] + recv_f[outer, 0]
            if y == BY - 1:
                tile = tile + recv_f[1 + x, EY - 1] + recv_f[outer, EY - 1]
            for c in range(3):
                out[c * BX + home(x), y : y + 1, :] = tile[c : c + 1]
    for copies in (p_copies, e_copies, f_copies):
        for copy in copies:
            copy.wait_send()


def unpack(packed, forces, energies):
    forces[...] = packed[0 : 3 * BX]
    energies[...] = packed[3 * BX :]


def solution(mesh):
    nx, ny = mesh.shape["gx"], mesh.shape["gy"]

    def body(positions, embed, counts, neighbours, w_one, bias_one, w_two, w_out):
        hbm = pl.BlockSpec(memory_space=pl.ANY)
        vmem = pl.BlockSpec(memory_space=pltpu.VMEM)
        packed = pl.pallas_call(
            functools.partial(kernel, nx, ny),
            out_shape=jax.ShapeDtypeStruct((4 * BX, BY, ATOMS), F32),
            in_specs=[hbm] * 8,
            out_specs=vmem,
            scratch_shapes=[
                pltpu.VMEM((EX, EY, ATOMS, FEAT), BF16),
                pltpu.VMEM((EX, EY, FEAT, ATOMS), BF16),
                pltpu.VMEM((EX, EY, 8, ATOMS), F32),
                pltpu.VMEM((EX, EY, 8, ATOMS), F32),
                pltpu.VMEM((EX, EY, 128, ATOMS), BF16),
                pltpu.VMEM((BX, BY, ATOMS, 128), BF16),
                pltpu.VMEM((GROUPS, 3, 2 * ATOMS, 2 * ATOMS), BF16),
                pltpu.VMEM((GROUPS, 2, ATOMS, 3 * ATOMS), BF16),
                pltpu.VMEM((GROUPS, 2 * ATOMS, FEAT), BF16),
                pltpu.VMEM((GROUPS, 2 * ATOMS, HID), F32),
                pltpu.VMEM((GROUPS, 2 * ATOMS, FEAT), BF16),
                pltpu.VMEM((EX, EY, 16, ATOMS), F32),
                pltpu.VMEM((EX, EY, 8, ATOMS), F32),
                pltpu.VMEM((EX, EY, 8, ATOMS), F32),
                pltpu.VMEM((3, BX, BY, ATOMS), F32),
                pltpu.SMEM((BX, BY), jnp.int32),
                pltpu.SMEM((BX, BY, 9), jnp.int32),
                pltpu.VMEM((FEAT, HID), BF16),
                pltpu.VMEM((1, HID), F32),
                pltpu.VMEM((HID, HID), BF16),
                pltpu.VMEM((1, HID), F32),
                pltpu.VMEM((HID, FEAT), BF16),
                pltpu.VMEM((HID, HID), BF16),
                pltpu.SemaphoreType.DMA((9,)),
                pltpu.SemaphoreType.DMA((8,)),
                pltpu.SemaphoreType.DMA((8,)),
                pltpu.SemaphoreType.DMA((14,)),
                pltpu.SemaphoreType.DMA((14,)),
                pltpu.SemaphoreType.DMA((8,)),
                pltpu.SemaphoreType.DMA((8,)),
            ],
            compiler_params=pltpu.CompilerParams(
                collective_id=0, has_side_effects=True, vmem_limit_bytes=60 * 1024 * 1024
            ),
        )(positions, embed, counts, neighbours, w_one, bias_one[None], w_two, w_out[None])
        forces, energies = pl.pallas_call(
            unpack,
            out_shape=(
                jax.ShapeDtypeStruct((3 * BX, BY, ATOMS), F32),
                jax.ShapeDtypeStruct((BX, BY, ATOMS), F32),
            ),
            in_specs=[vmem],
            out_specs=(vmem, vmem),
        )(packed)
        return forces.reshape(3, BX, BY, ATOMS), energies

    in_specs = (
        P(None, "gx", "gy", None),
        P("gx", "gy", None, None),
        P("gx", "gy"),
        P("gx", "gy", None),
        P(),
        P(),
        P(),
        P(),
    )
    out_specs = (P(None, "gx", "gy", None), P("gx", "gy", None))
    return jax.shard_map(body, mesh=mesh, in_specs=in_specs, out_specs=out_specs, check_vma=False)
```

```python
import functools

import jax
import jax.numpy as jnp
from jax import lax
from jax.experimental import pallas as pl
from jax.experimental.pallas import tpu as pltpu
from jax.sharding import PartitionSpec as P

MESH = pl.DeviceIdType.MESH
F32 = jnp.float32
BF16 = jnp.bfloat16
radius = 0.4
INV = 1.0 / (radius * radius)
KAPPA = 1.4426950408889634 / (2.0 * radius * radius)
OFF = -30000.0
BX, BY, ATOMS, FEAT, HID = 2, 8, 128, 256, 256
EX, EY = BX + 2, BY + 2
GROUPS = BX * BY // 2
DIRS = ((-1, 0), (-1, -1), (-1, 1), (0, -1), (0, 1), (1, 0), (1, -1), (1, 1))


def rim(step, size):
    return pl.ds(1, 1) if step < 0 else pl.ds(size, 1) if step > 0 else pl.ds(1, size)


def ghost(step, size):
    return pl.ds(0, 1) if step < 0 else pl.ds(size + 1, 1) if step > 0 else pl.ds(1, size)


def split3(value):
    high = value.astype(BF16).astype(F32)
    rest = value - high
    middle = rest.astype(BF16).astype(F32)
    return high, middle, rest - middle


def kernel(
    nx, ny,
    pos_hbm, emb_hbm, cnt_hbm, nbr_hbm, w1_hbm, b1_hbm, w2_hbm, wo_hbm,
    out,
    emb, emb_t, raw, glob, rows, cols, w_mid, w_side, feat, act, grad, sums, ghost_f, recv_f,
    pos, cnt, nbr, w1, b1, w2, wo, w1_t, w2_t,
    local_sem, p_send, p_recv, e_send, e_recv, f_send, f_recv,
):
    gx, gy = lax.axis_index("gx"), lax.axis_index("gy")
    odd = lax.rem(gx, 2)
    sign = 1 - 2 * odd
    turn = sign.astype(F32)

    def peer(side, dy):
        return (lax.rem(gx + side * sign + nx, nx), lax.rem(gy + (dy + ny), ny))

    def home(x):
        return x + odd * (1 - 2 * x)

    barrier = pltpu.get_barrier_semaphore()
    for side, dy in DIRS:
        pl.semaphore_signal(barrier, inc=1, device_id=peer(side, dy), device_id_type=MESH)

    loads = [
        pltpu.make_async_copy(pos_hbm, pos, local_sem.at[0]),
        pltpu.make_async_copy(cnt_hbm, cnt, local_sem.at[7]),
        pltpu.make_async_copy(emb_hbm.at[home(0)], emb.at[1, pl.ds(1, BY)], local_sem.at[1]),
        pltpu.make_async_copy(emb_hbm.at[home(1)], emb.at[2, pl.ds(1, BY)], local_sem.at[6]),
        pltpu.make_async_copy(w1_hbm, w1, local_sem.at[2]),
        pltpu.make_async_copy(b1_hbm, b1, local_sem.at[3]),
        pltpu.make_async_copy(w2_hbm, w2, local_sem.at[4]),
        pltpu.make_async_copy(wo_hbm, wo, local_sem.at[5]),
        pltpu.make_async_copy(nbr_hbm, nbr, local_sem.at[8]),
    ]
    for load in loads:
        load.start()

    def send(src, dst, send_sem, recv_sem, i, target):
        return pltpu.make_async_remote_copy(
            src_ref=src, dst_ref=dst, send_sem=send_sem.at[i], recv_sem=recv_sem.at[i],
            device_id=target, device_id_type=MESH,
        )

    p_copies = [
        send(raw.at[rim(side, BX), rim(dy, BY)], raw.at[ghost(side, BX), ghost(-dy, BY)],
             p_send, p_recv, i, peer(side, dy))
        for i, (side, dy) in enumerate(DIRS)
    ]
    f_copies = [
        send(ghost_f.at[ghost(side, BX), ghost(dy, BY)], recv_f.at[ghost(side, BX), ghost(-dy, BY)],
             f_send, f_recv, i, peer(side, dy))
        for i, (side, dy) in enumerate(DIRS)
    ]
    lo, hi, all_y = pl.ds(1, 1), pl.ds(BY, 1), pl.ds(1, BY)
    west, east = pl.ds(0, 1), pl.ds(BY + 1, 1)
    r0, r1, r2, r3 = (pl.ds(i, 1) for i in range(EX))
    routes = (
        (r2, lo, r2, east, 0, -1),
        (r2, hi, r2, west, 0, 1),
        (r1, lo, r1, east, 0, -1),
        (r1, hi, r1, west, 0, 1),
        (r1, lo, r0, lo, -1, 0),
        (r1, hi, r0, hi, -1, 0),
        (r1, pl.ds(2, 2), r0, pl.ds(2, 2), -1, 0),
        (r1, pl.ds(BY - 2, 2), r0, pl.ds(BY - 2, 2), -1, 0),
        (r1, pl.ds(4, BY - 6), r0, pl.ds(4, BY - 6), -1, 0),
        (r2, all_y, r3, all_y, 1, 0),
        (r2, west, r3, west, 1, 0),
        (r2, east, r3, east, 1, 0),
        (r0, lo, r0, east, 0, -1),
        (r0, hi, r0, west, 0, 1),
    )
    e_copies = [
        send(emb.at[sx, sy], emb.at[tx, ty], e_send, e_recv, i, peer(side, dy))
        for i, (sx, sy, tx, ty, side, dy) in enumerate(routes)
    ]
    near_cols, far_cols, far_edges, far_outer, far_inner, near_in = (
        e_copies[i:j] for i, j in ((0, 2), (2, 4), (4, 6), (6, 8), (8, 9), (9, 10))
    )
    near_relay, far_relay = e_copies[10:12], e_copies[12:14]

    def start(copies):
        for copy in copies:
            copy.start()

    def arrive(copies):
        for copy in copies:
            copy.wait_recv()

    loads[0].wait()
    loads[1].wait()
    lane = lax.broadcasted_iota(jnp.int32, (1, ATOMS), 1)
    for x in range(BX):
        for y in range(BY):
            tile = jnp.concatenate(
                [pos[c, home(x), y : y + 1, :] for c in range(3)]
                + [jnp.where(lane < cnt[home(x), y], 0.0, OFF).astype(F32)]
                + [jnp.zeros((4, ATOMS), F32)],
                axis=0,
            )
            raw[1 + x, 1 + y] = tile

    pl.semaphore_wait(barrier, len(DIRS))
    start(p_copies)
    loads[2].wait()
    loads[3].wait()
    start(near_cols + far_edges + near_in + far_cols + far_outer + far_inner)

    row = lax.broadcasted_iota(jnp.int32, (8, ATOMS), 0)
    mark = lax.broadcasted_iota(jnp.int32, (80, ATOMS), 0)

    def make_rows(ex, ey):
        tile = raw[ex, ey]
        place = tile + jnp.where(
            row == 0, turn * (ex - 1.5), jnp.where(row == 1, ey - 5.0, jnp.where(row == 2, -0.5, 0.0))
        )
        glob[ex, ey] = place
        square = place * place
        bias = place[3:4] - KAPPA * (square[0:1] + square[1:2] + square[2:3])
        full = jnp.where(row < 3, place, jnp.where(row == 3, bias, jnp.where(row == 4, 1.0, 0.0)))
        high, middle, low = split3(full)
        one_hot = jnp.where(mark == (ex + odd * (EX - 1 - 2 * ex)) * EY + ey, 1.0, 0.0)
        rows[ex, ey] = jnp.concatenate([high, middle, low, high, middle, high, one_hot], axis=0).astype(BF16)
        return place, bias

    def make_cols(x, y, place, bias):
        full = jnp.where(row < 3, (2.0 * KAPPA) * place, jnp.where(row == 3, 1.0, jnp.where(row == 4, bias, 0.0)))
        high, middle, low = split3(full)
        present = mark == nbr[home(x), y, 0]
        for k in range(1, 9):
            present = jnp.logical_or(present, mark == nbr[home(x), y, k])
        missing = jnp.where(present, 0.0, OFF)
        stack = jnp.concatenate([high, high, high, middle, middle, low, missing], axis=0)
        cols[x, y] = jnp.transpose(stack).astype(BF16)

    def flip(ex, ey):
        emb_t[ex, ey] = jnp.transpose(emb[ex, ey])

    loads[8].wait()
    def spot(g):
        return g // (BY // 2), 2 * (g % (BY // 2))

    def row_block(x, y, steps, count, height=128):
        return jnp.concatenate([rows[x + dr, y + c, 0:height] for dr in steps for c in range(count)], axis=1)

    def middle_weights(g, steps):
        x, y = spot(g)
        left = jnp.concatenate([cols[x, y], cols[x, y + 1]], axis=0)
        for dr in steps:
            power = jnp.dot(left, row_block(x, y + 1, (dr,), 2), preferred_element_type=F32)
            w_mid[g, dr] = jnp.exp2(power).astype(BF16)

    def inner_sides(g):
        _, y = spot(g)
        return [b for b in range(2) if y + 3 * b not in (0, EY - 1)]

    def side_weights(g, b, steps):
        x, y = spot(g)
        power = jnp.dot(cols[x, y + b], row_block(x, y + 3 * b, steps, 1), preferred_element_type=F32)
        w_side[g, b, :, steps[0] * ATOMS : (steps[-1] + 1) * ATOMS] = jnp.exp2(power).astype(BF16)

    def late_sides(g):
        for b in range(2):
            side_weights(g, b, (ghost_step(g),) if b in inner_sides(g) else (0, 1, 2))

    def side_part(g, b, steps):
        x, y = spot(g)
        block = emb[x + steps[0] : x + steps[-1] + 1, y + 3 * b].reshape(len(steps) * ATOMS, FEAT)
        share = w_side[g, b, :, steps[0] * ATOMS : (steps[-1] + 1) * ATOMS]
        return jnp.dot(share, block, preferred_element_type=F32)

    def middle_part(g, dr):
        x, y = spot(g)
        block = emb[x + dr, y + 1 : y + 3].reshape(2 * ATOMS, FEAT)
        return jnp.dot(w_mid[g, dr], block, preferred_element_type=F32)

    def own_steps(g):
        return (1, 2) if g < GROUPS // 2 else (0, 1)

    def ghost_step(g):
        return 0 if g < GROUPS // 2 else 2

    def features_of(g):
        total = act[g] + middle_part(g, ghost_step(g))
        for b in range(2):
            part = side_part(g, b, (ghost_step(g),) if b in inner_sides(g) else (0, 1, 2))
            half = slice(b * ATOMS, (b + 1) * ATOMS)
            feat[g, half] = (total[half] + part).astype(BF16)

    for x in range(BX):
        for y in range(BY):
            place, bias = make_rows(1 + x, 1 + y)
            make_cols(x, y, place, bias)
    for load in loads[4:8]:
        load.wait()
    w1_t[...] = jnp.transpose(w1[...])
    w2_t[...] = jnp.transpose(w2[...])
    for x in range(BX):
        for y in range(BY):
            flip(1 + x, 1 + y)
    sums[...] = jnp.zeros_like(sums)

    for g in range(GROUPS):
        middle_weights(g, own_steps(g))
        for b in inner_sides(g):
            side_weights(g, b, own_steps(g))
    for g in range(GROUPS):
        first, second = own_steps(g)
        total = middle_part(g, first) + middle_part(g, second)
        for b in range(2):
            half = slice(b * ATOMS, (b + 1) * ATOMS)
            inner = b in inner_sides(g)
            act[g, half] = total[half] + side_part(g, b, own_steps(g)) if inner else total[half]

    out_row = wo[...]
    bias_row = b1[...]

    def network(groups):
        for g in groups:
            act[g] = jnp.tanh(jnp.dot(feat[g], w1[...], preferred_element_type=F32) + bias_row)
        for g in groups:
            x, y = spot(g)
            two = jnp.tanh(jnp.dot(act[g].astype(BF16), w2[...], preferred_element_type=F32))
            scaled = two * out_row
            halves = scaled[:, :128] + scaled[:, 128:]
            for b in range(2):
                turned = jnp.transpose(halves[b * ATOMS : (b + 1) * ATOMS])
                energy = jnp.sum(turned, axis=0, keepdims=True)
                out[3 * BX + home(x), y + b : y + b + 1, :] = jnp.where(lane < cnt[home(x), y + b], energy, 0.0)
            feat[g] = (out_row * (1.0 - two * two)).astype(BF16)
        for g in groups:
            one = act[g]
            back = jnp.dot(feat[g], w2_t[...], preferred_element_type=F32) * (1.0 - one * one)
            grad[g] = back.astype(BF16)
        for g in groups:
            grad[g] = jnp.dot(grad[g], w1_t[...], preferred_element_type=F32).astype(BF16)

    def ghost_units(g):
        _, y = spot(g)
        units = [(g, 0, 2, (ghost_step(g),), 1, 2)]
        units += [(g, b, 1, (ghost_step(g),), 3 * b, 1) for b in range(2)]
        return units + [(g, b, 1, own_steps(g), 3 * b, 1) for b in range(2) if y + 3 * b in (0, EY - 1)]

    def inner_units(g):
        _, y = spot(g)
        units = [(g, 0, 2, (dr,), 1, 2) for dr in own_steps(g)]
        return units + [(g, b, 1, own_steps(g), 3 * b, 1) for b in range(2) if y + 3 * b not in (0, EY - 1)]

    def project(unit):
        g, first, slots, steps, col, count = unit
        x, y = spot(g)
        right = jnp.concatenate([emb_t[x + dr, y + col + c] for dr in steps for c in range(count)], axis=1)
        slope = grad[g, first * ATOMS : (first + slots) * ATOMS]
        return jnp.dot(slope, right, preferred_element_type=F32)

    def strengthen(unit):
        g, first, slots, steps, col, count = unit
        projected = project(unit).astype(BF16)
        if slots == 2:
            w_mid[g, steps[0]] = projected * w_mid[g, steps[0]]
        else:
            part = slice(steps[0] * ATOMS, (steps[-1] + 1) * ATOMS)
            w_side[g, first, :, part] = projected * w_side[g, first, :, part]

    def spread(unit):
        g, first, slots, steps, col, count = unit
        x, y = spot(g)
        if slots == 2:
            strength = w_mid[g, steps[0]]
        else:
            strength = w_side[g, first, :, steps[0] * ATOMS : (steps[-1] + 1) * ATOMS]
        other = row_block(x, y + col, steps, count, 16)
        part = lax.dot_general(strength, other, (((1,), (1,)), ((), ())), preferred_element_type=F32)
        own = row_block(x, y + 1 + first, (1,), slots, 16)
        pushed = jnp.dot(own, strength, preferred_element_type=F32)
        spots = [(x + dr, y + col + c) for dr in steps for c in range(count)]
        for i, (ex, ey) in enumerate(spots):
            sums[ex, ey] += pushed[:, i * ATOMS : (i + 1) * ATOMS]
        return part

    def forces_of(units):
        for unit in units:
            strengthen(unit)
        gathered = {}
        for unit in units:
            part = spread(unit)
            g, first, slots = unit[:3]
            for b in range(slots):
                piece = part[b * ATOMS : (b + 1) * ATOMS]
                key = (g, first + b)
                gathered[key] = piece if key not in gathered else gathered[key] + piece
        for (g, b), total in gathered.items():
            x, y = spot(g)
            sums[x + 1, y + 1 + b] += jnp.transpose(total)

    def force_tile(ex, ey):
        moment = sums[ex, ey, 0:8] + sums[ex, ey, 8:16]
        return (glob[ex, ey] * moment[4:5] - moment) * INV

    far, near = range(GROUPS // 2), range(GROUPS // 2, GROUPS)
    arrive(p_copies[3:8])
    for ey in range(EY):
        make_rows(EX - 1, ey)
    for ex in range(1, EX - 1):
        make_rows(ex, 0)
        make_rows(ex, EY - 1)
    for g in near:
        middle_weights(g, (2,))
        late_sides(g)
    arrive(near_cols)
    start(near_relay)
    arrive(p_copies[0:3])
    for ey in range(EY):
        make_rows(0, ey)
    arrive(far_edges)
    start(far_relay)
    arrive(near_in)
    for ey in range(1, EY - 1):
        flip(EX - 1, ey)
    inside, outside = (5, 6), (4, 7)
    for g in inside:
        features_of(g)
    network(inside)
    for g in far:
        middle_weights(g, (0,))
        late_sides(g)
    arrive(far_cols + near_relay)
    for ex in range(1, EX - 1):
        flip(ex, 0)
        flip(ex, EY - 1)
    flip(EX - 1, 0)
    flip(EX - 1, EY - 1)
    for g in outside:
        features_of(g)
    network(outside)
    forces_of([unit for g in inside + outside for unit in ghost_units(g)])
    for ey in range(EY):
        ghost_f[EX - 1, ey] = force_tile(EX - 1, ey)
    start(f_copies[5:8])

    arrive(far_outer + far_relay)
    for ey in (0, 1, 2, 3, 6, 7, 8, 9):
        flip(0, ey)
    for g in (0, 3):
        features_of(g)
    network((0, 3))
    forces_of([unit for g in (0, 3) for unit in ghost_units(g)])
    for ey in (0, EY - 1):
        for ex in range(EX - 1):
            ghost_f[ex, ey] = force_tile(ex, ey)
    start(f_copies[1:5])
    arrive(far_inner)
    for ey in (4, 5):
        flip(0, ey)
    for g in (1, 2):
        features_of(g)
    network((1, 2))
    forces_of([unit for g in (1, 2) for unit in ghost_units(g)])
    for ey in range(1, EY - 1):
        ghost_f[0, ey] = force_tile(0, ey)
    start(f_copies[0:1])
    forces_of([unit for g in near for unit in inner_units(g)])
    forces_of([unit for g in far for unit in inner_units(g)])
    for x in range(BX):
        for y in range(BY):
            sums[1 + x, 1 + y, 0:8] = force_tile(1 + x, 1 + y)
    arrive(f_copies)
    for x in range(BX):
        outer = 0 if x == 0 else EX - 1
        for y in range(BY):
            tile = sums[1 + x, 1 + y, 0:8] + recv_f[outer, 1 + y]
            if y == 0:
                tile = tile + recv_f[1 + x, 0] + recv_f[outer, 0]
            if y == BY - 1:
                tile = tile + recv_f[1 + x, EY - 1] + recv_f[outer, EY - 1]
            for c in range(3):
                out[c * BX + home(x), y : y + 1, :] = tile[c : c + 1]
    for copies in (p_copies, e_copies, f_copies):
        for copy in copies:
            copy.wait_send()


def unpack(packed, forces, energies):
    forces[...] = packed[0 : 3 * BX]
    energies[...] = packed[3 * BX :]


def solution(mesh):
    nx, ny = mesh.shape["gx"], mesh.shape["gy"]

    def body(positions, embed, counts, neighbours, w_one, bias_one, w_two, w_out):
        hbm = pl.BlockSpec(memory_space=pl.ANY)
        vmem = pl.BlockSpec(memory_space=pltpu.VMEM)
        packed = pl.pallas_call(
            functools.partial(kernel, nx, ny),
            out_shape=pltpu.VMEM((4 * BX, BY, ATOMS), F32),
            in_specs=[hbm] * 8,
            out_specs=vmem,
            scratch_shapes=[
                pltpu.VMEM((EX, EY, ATOMS, FEAT), BF16),
                pltpu.VMEM((EX, EY, FEAT, ATOMS), BF16),
                pltpu.VMEM((EX, EY, 8, ATOMS), F32),
                pltpu.VMEM((EX, EY, 8, ATOMS), F32),
                pltpu.VMEM((EX, EY, 128, ATOMS), BF16),
                pltpu.VMEM((BX, BY, ATOMS, 128), BF16),
                pltpu.VMEM((GROUPS, 3, 2 * ATOMS, 2 * ATOMS), BF16),
                pltpu.VMEM((GROUPS, 2, ATOMS, 3 * ATOMS), BF16),
                pltpu.VMEM((GROUPS, 2 * ATOMS, FEAT), BF16),
                pltpu.VMEM((GROUPS, 2 * ATOMS, HID), F32),
                pltpu.VMEM((GROUPS, 2 * ATOMS, FEAT), BF16),
                pltpu.VMEM((EX, EY, 16, ATOMS), F32),
                pltpu.VMEM((EX, EY, 8, ATOMS), F32),
                pltpu.VMEM((EX, EY, 8, ATOMS), F32),
                pltpu.VMEM((3, BX, BY, ATOMS), F32),
                pltpu.SMEM((BX, BY), jnp.int32),
                pltpu.SMEM((BX, BY, 9), jnp.int32),
                pltpu.VMEM((FEAT, HID), BF16),
                pltpu.VMEM((1, HID), F32),
                pltpu.VMEM((HID, HID), BF16),
                pltpu.VMEM((1, HID), F32),
                pltpu.VMEM((HID, FEAT), BF16),
                pltpu.VMEM((HID, HID), BF16),
                pltpu.SemaphoreType.DMA((9,)),
                pltpu.SemaphoreType.DMA((8,)),
                pltpu.SemaphoreType.DMA((8,)),
                pltpu.SemaphoreType.DMA((14,)),
                pltpu.SemaphoreType.DMA((14,)),
                pltpu.SemaphoreType.DMA((8,)),
                pltpu.SemaphoreType.DMA((8,)),
            ],
            compiler_params=pltpu.CompilerParams(
                collective_id=0, has_side_effects=True, vmem_limit_bytes=60 * 1024 * 1024
            ),
        )(positions, embed, counts, neighbours, w_one, bias_one[None], w_two, w_out[None])
        forces, energies = pl.pallas_call(
            unpack,
            out_shape=(
                jax.ShapeDtypeStruct((3 * BX, BY, ATOMS), F32),
                jax.ShapeDtypeStruct((BX, BY, ATOMS), F32),
            ),
            in_specs=[vmem],
            out_specs=(vmem, vmem),
        )(pltpu.with_memory_space_constraint(packed, pltpu.VMEM))
        return forces.reshape(3, BX, BY, ATOMS), energies

    in_specs = (
        P(None, "gx", "gy", None),
        P("gx", "gy", None, None),
        P("gx", "gy"),
        P("gx", "gy", None),
        P(),
        P(),
        P(),
        P(),
    )
    out_specs = (P(None, "gx", "gy", None), P("gx", "gy", None))
    return jax.shard_map(body, mesh=mesh, in_specs=in_specs, out_specs=out_specs, check_vma=False)
```

```python
import functools

import jax
import jax.numpy as jnp
from jax import lax
from jax.experimental import pallas as pl
from jax.experimental.pallas import tpu as pltpu
from jax.sharding import PartitionSpec as P

MESH = pl.DeviceIdType.MESH
F32 = jnp.float32
BF16 = jnp.bfloat16
radius = 0.4
INV = 1.0 / (radius * radius)
KAPPA = 1.4426950408889634 / (2.0 * radius * radius)
OFF = -30000.0
BX, BY, ATOMS, FEAT, HID = 2, 8, 128, 256, 256
EX, EY = BX + 2, BY + 2
GROUPS = BX * BY // 2
DIRS = ((-1, 0), (-1, -1), (-1, 1), (0, -1), (0, 1), (1, 0), (1, -1), (1, 1))


def rim(step, size):
    return pl.ds(1, 1) if step < 0 else pl.ds(size, 1) if step > 0 else pl.ds(1, size)


def ghost(step, size):
    return pl.ds(0, 1) if step < 0 else pl.ds(size + 1, 1) if step > 0 else pl.ds(1, size)


def split3(value):
    high = value.astype(BF16).astype(F32)
    rest = value - high
    middle = rest.astype(BF16).astype(F32)
    return high, middle, rest - middle


def kernel(
    nx, ny,
    pos_hbm, emb_hbm, cnt_hbm, nbr_hbm, w1_hbm, b1_hbm, w2_hbm, wo_hbm,
    out,
    emb, emb_t, raw, glob, rows, cols, w_mid, w_side, feat, act, grad, shares, sums, ghost_f, recv_f,
    pos, cnt, nbr, w1, b1, w2, wo, w1_t, w2_t,
    local_sem, p_send, p_recv, e_send, e_recv, f_send, f_recv,
):
    gx, gy = lax.axis_index("gx"), lax.axis_index("gy")
    odd = lax.rem(gx, 2)
    sign = 1 - 2 * odd
    turn = sign.astype(F32)

    def peer(side, dy):
        return (lax.rem(gx + side * sign + nx, nx), lax.rem(gy + (dy + ny), ny))

    def home(x):
        return x + odd * (1 - 2 * x)

    barrier = pltpu.get_barrier_semaphore()
    for side, dy in DIRS:
        pl.semaphore_signal(barrier, inc=1, device_id=peer(side, dy), device_id_type=MESH)

    loads = [
        pltpu.make_async_copy(pos_hbm, pos, local_sem.at[0]),
        pltpu.make_async_copy(cnt_hbm, cnt, local_sem.at[7]),
        pltpu.make_async_copy(emb_hbm.at[home(0)], emb.at[1, pl.ds(1, BY)], local_sem.at[1]),
        pltpu.make_async_copy(emb_hbm.at[home(1)], emb.at[2, pl.ds(1, BY)], local_sem.at[6]),
        pltpu.make_async_copy(w1_hbm, w1, local_sem.at[2]),
        pltpu.make_async_copy(b1_hbm, b1, local_sem.at[3]),
        pltpu.make_async_copy(w2_hbm, w2, local_sem.at[4]),
        pltpu.make_async_copy(wo_hbm, wo, local_sem.at[5]),
        pltpu.make_async_copy(nbr_hbm, nbr, local_sem.at[8]),
    ]
    for load in loads:
        load.start()

    def send(src, dst, send_sem, recv_sem, i, target):
        return pltpu.make_async_remote_copy(
            src_ref=src, dst_ref=dst, send_sem=send_sem.at[i], recv_sem=recv_sem.at[i],
            device_id=target, device_id_type=MESH,
        )

    p_copies = [
        send(raw.at[rim(side, BX), rim(dy, BY)], raw.at[ghost(side, BX), ghost(-dy, BY)],
             p_send, p_recv, i, peer(side, dy))
        for i, (side, dy) in enumerate(DIRS)
    ]
    f_copies = [
        send(ghost_f.at[ghost(side, BX), ghost(dy, BY)], recv_f.at[ghost(side, BX), ghost(-dy, BY)],
             f_send, f_recv, i, peer(side, dy))
        for i, (side, dy) in enumerate(DIRS)
    ]
    lo, hi, all_y = pl.ds(1, 1), pl.ds(BY, 1), pl.ds(1, BY)
    west, east = pl.ds(0, 1), pl.ds(BY + 1, 1)
    r0, r1, r2, r3 = (pl.ds(i, 1) for i in range(EX))
    routes = (
        (r2, lo, r2, east, 0, -1),
        (r2, hi, r2, west, 0, 1),
        (r1, lo, r1, east, 0, -1),
        (r1, hi, r1, west, 0, 1),
        (r1, lo, r0, lo, -1, 0),
        (r1, hi, r0, hi, -1, 0),
        (r1, pl.ds(2, 2), r0, pl.ds(2, 2), -1, 0),
        (r1, pl.ds(BY - 2, 2), r0, pl.ds(BY - 2, 2), -1, 0),
        (r1, pl.ds(4, BY - 6), r0, pl.ds(4, BY - 6), -1, 0),
        (r2, all_y, r3, all_y, 1, 0),
        (r2, west, r3, west, 1, 0),
        (r2, east, r3, east, 1, 0),
        (r0, lo, r0, east, 0, -1),
        (r0, hi, r0, west, 0, 1),
    )
    e_copies = [
        send(emb.at[sx, sy], emb.at[tx, ty], e_send, e_recv, i, peer(side, dy))
        for i, (sx, sy, tx, ty, side, dy) in enumerate(routes)
    ]
    near_cols, far_cols, far_edges, far_outer, far_inner, near_in = (
        e_copies[i:j] for i, j in ((0, 2), (2, 4), (4, 6), (6, 8), (8, 9), (9, 10))
    )
    near_relay, far_relay = e_copies[10:12], e_copies[12:14]

    def start(copies):
        for copy in copies:
            copy.start()

    def arrive(copies):
        for copy in copies:
            copy.wait_recv()

    loads[0].wait()
    loads[1].wait()
    lane = lax.broadcasted_iota(jnp.int32, (1, ATOMS), 1)
    for x in range(BX):
        for y in range(BY):
            tile = jnp.concatenate(
                [pos[c, home(x), y : y + 1, :] for c in range(3)]
                + [jnp.where(lane < cnt[home(x), y], 0.0, OFF).astype(F32)]
                + [jnp.zeros((4, ATOMS), F32)],
                axis=0,
            )
            raw[1 + x, 1 + y] = tile

    pl.semaphore_wait(barrier, len(DIRS))
    start(p_copies)
    loads[2].wait()
    loads[3].wait()
    start(near_cols + far_edges + near_in + far_cols + far_outer + far_inner)

    row = lax.broadcasted_iota(jnp.int32, (8, ATOMS), 0)
    mark = lax.broadcasted_iota(jnp.int32, (80, ATOMS), 0)

    def make_rows(ex, ey):
        tile = raw[ex, ey]
        place = tile + jnp.where(
            row == 0, turn * (ex - 1.5), jnp.where(row == 1, ey - 5.0, jnp.where(row == 2, -0.5, 0.0))
        )
        glob[ex, ey] = place
        square = place * place
        bias = place[3:4] - KAPPA * (square[0:1] + square[1:2] + square[2:3])
        full = jnp.where(row < 3, place, jnp.where(row == 3, bias, jnp.where(row == 4, 1.0, 0.0)))
        high, middle, low = split3(full)
        one_hot = jnp.where(mark == (ex + odd * (EX - 1 - 2 * ex)) * EY + ey, 1.0, 0.0)
        rows[ex, ey] = jnp.concatenate([high, middle, low, high, middle, high, one_hot], axis=0).astype(BF16)
        return place, bias

    def make_cols(x, y, place, bias):
        full = jnp.where(row < 3, (2.0 * KAPPA) * place, jnp.where(row == 3, 1.0, jnp.where(row == 4, bias, 0.0)))
        high, middle, low = split3(full)
        present = mark == nbr[home(x), y, 0]
        for k in range(1, 9):
            present = jnp.logical_or(present, mark == nbr[home(x), y, k])
        missing = jnp.where(present, 0.0, OFF)
        stack = jnp.concatenate([high, high, high, middle, middle, low, missing], axis=0)
        cols[x, y] = jnp.transpose(stack).astype(BF16)

    def flip(ex, ey):
        emb_t[ex, ey] = jnp.transpose(emb[ex, ey])

    loads[8].wait()
    def spot(g):
        return g // (BY // 2), 2 * (g % (BY // 2))

    def row_block(x, y, steps, count, height=128):
        return jnp.concatenate([rows[x + dr, y + c, 0:height] for dr in steps for c in range(count)], axis=1)

    def middle_weights(g, steps):
        x, y = spot(g)
        left = jnp.concatenate([cols[x, y], cols[x, y + 1]], axis=0)
        for dr in steps:
            power = jnp.dot(left, row_block(x, y + 1, (dr,), 2), preferred_element_type=F32)
            w_mid[g, dr] = jnp.exp2(power).astype(BF16)

    def inner_sides(g):
        _, y = spot(g)
        return [b for b in range(2) if y + 3 * b not in (0, EY - 1)]

    def side_weights(g, b, steps):
        x, y = spot(g)
        power = jnp.dot(cols[x, y + b], row_block(x, y + 3 * b, steps, 1), preferred_element_type=F32)
        w_side[g, b, :, steps[0] * ATOMS : (steps[-1] + 1) * ATOMS] = jnp.exp2(power).astype(BF16)

    def late_sides(g):
        for b in range(2):
            side_weights(g, b, (ghost_step(g),) if b in inner_sides(g) else (0, 1, 2))

    def side_part(g, b, steps):
        x, y = spot(g)
        block = emb[x + steps[0] : x + steps[-1] + 1, y + 3 * b].reshape(len(steps) * ATOMS, FEAT)
        share = w_side[g, b, :, steps[0] * ATOMS : (steps[-1] + 1) * ATOMS]
        return jnp.dot(share, block, preferred_element_type=F32)

    def middle_part(g, dr):
        x, y = spot(g)
        block = emb[x + dr, y + 1 : y + 3].reshape(2 * ATOMS, FEAT)
        return jnp.dot(w_mid[g, dr], block, preferred_element_type=F32)

    def own_steps(g):
        return (1, 2) if g < GROUPS // 2 else (0, 1)

    def ghost_step(g):
        return 0 if g < GROUPS // 2 else 2

    def features_of(g):
        total = act[g] + middle_part(g, ghost_step(g))
        for b in range(2):
            part = side_part(g, b, (ghost_step(g),) if b in inner_sides(g) else (0, 1, 2))
            half = slice(b * ATOMS, (b + 1) * ATOMS)
            feat[g, half] = (total[half] + part).astype(BF16)

    for x in range(BX):
        for y in range(BY):
            place, bias = make_rows(1 + x, 1 + y)
            make_cols(x, y, place, bias)
    for load in loads[4:8]:
        load.wait()
    w1_t[...] = jnp.transpose(w1[...])
    w2_t[...] = jnp.transpose(w2[...])
    for x in range(BX):
        for y in range(BY):
            flip(1 + x, 1 + y)
    sums[...] = jnp.zeros_like(sums)

    for g in range(GROUPS):
        middle_weights(g, own_steps(g))
        for b in inner_sides(g):
            side_weights(g, b, own_steps(g))
    for g in range(GROUPS):
        first, second = own_steps(g)
        total = middle_part(g, first) + middle_part(g, second)
        for b in range(2):
            half = slice(b * ATOMS, (b + 1) * ATOMS)
            inner = b in inner_sides(g)
            act[g, half] = total[half] + side_part(g, b, own_steps(g)) if inner else total[half]

    out_row = wo[...]
    bias_row = b1[...]

    def network(groups):
        for g in groups:
            act[g] = jnp.tanh(jnp.dot(feat[g], w1[...], preferred_element_type=F32) + bias_row)
        for g in groups:
            two = jnp.tanh(jnp.dot(act[g].astype(BF16), w2[...], preferred_element_type=F32))
            scaled = two * out_row
            halves = scaled[:, :128] + scaled[:, 128:]
            shares[g] = halves
            feat[g] = (out_row * (1.0 - two * two)).astype(BF16)
        for g in groups:
            one = act[g]
            back = jnp.dot(feat[g], w2_t[...], preferred_element_type=F32) * (1.0 - one * one)
            grad[g] = back.astype(BF16)
        for g in groups:
            grad[g] = jnp.dot(grad[g], w1_t[...], preferred_element_type=F32).astype(BF16)

    def ghost_units(g):
        _, y = spot(g)
        units = [(g, 0, 2, (ghost_step(g),), 1, 2)]
        units += [(g, b, 1, (ghost_step(g),), 3 * b, 1) for b in range(2)]
        return units + [(g, b, 1, own_steps(g), 3 * b, 1) for b in range(2) if y + 3 * b in (0, EY - 1)]

    def inner_units(g):
        _, y = spot(g)
        units = [(g, 0, 2, (dr,), 1, 2) for dr in own_steps(g)]
        return units + [(g, b, 1, own_steps(g), 3 * b, 1) for b in range(2) if y + 3 * b not in (0, EY - 1)]

    def project(unit):
        g, first, slots, steps, col, count = unit
        x, y = spot(g)
        right = jnp.concatenate([emb_t[x + dr, y + col + c] for dr in steps for c in range(count)], axis=1)
        slope = grad[g, first * ATOMS : (first + slots) * ATOMS]
        return jnp.dot(slope, right, preferred_element_type=F32)

    def strengthen(unit):
        g, first, slots, steps, col, count = unit
        projected = project(unit).astype(BF16)
        if slots == 2:
            w_mid[g, steps[0]] = projected * w_mid[g, steps[0]]
        else:
            part = slice(steps[0] * ATOMS, (steps[-1] + 1) * ATOMS)
            w_side[g, first, :, part] = projected * w_side[g, first, :, part]

    def spread(unit):
        g, first, slots, steps, col, count = unit
        x, y = spot(g)
        if slots == 2:
            strength = w_mid[g, steps[0]]
        else:
            strength = w_side[g, first, :, steps[0] * ATOMS : (steps[-1] + 1) * ATOMS]
        other = row_block(x, y + col, steps, count, 16)
        part = lax.dot_general(strength, other, (((1,), (1,)), ((), ())), preferred_element_type=F32)
        own = row_block(x, y + 1 + first, (1,), slots, 16)
        pushed = jnp.dot(own, strength, preferred_element_type=F32)
        spots = [(x + dr, y + col + c) for dr in steps for c in range(count)]
        for i, (ex, ey) in enumerate(spots):
            sums[ex, ey] += pushed[:, i * ATOMS : (i + 1) * ATOMS]
        return part

    def forces_of(units):
        for unit in units:
            strengthen(unit)
        gathered = {}
        for unit in units:
            part = spread(unit)
            g, first, slots = unit[:3]
            for b in range(slots):
                piece = part[b * ATOMS : (b + 1) * ATOMS]
                key = (g, first + b)
                gathered[key] = piece if key not in gathered else gathered[key] + piece
        return gathered

    def settle(gathered):
        for (g, b), total in gathered.items():
            x, y = spot(g)
            sums[x + 1, y + 1 + b] += jnp.transpose(total)

    def force_tile(ex, ey):
        moment = sums[ex, ey, 0:8] + sums[ex, ey, 8:16]
        return (glob[ex, ey] * moment[4:5] - moment) * INV

    far, near = range(GROUPS // 2), range(GROUPS // 2, GROUPS)
    arrive(p_copies[3:8])
    for ey in range(EY):
        make_rows(EX - 1, ey)
    for ex in range(1, EX - 1):
        make_rows(ex, 0)
        make_rows(ex, EY - 1)
    for g in near:
        middle_weights(g, (2,))
        late_sides(g)
    arrive(near_cols)
    start(near_relay)
    arrive(p_copies[0:3])
    for ey in range(EY):
        make_rows(0, ey)
    arrive(far_edges)
    start(far_relay)
    arrive(near_in)
    for ey in range(1, EY - 1):
        flip(EX - 1, ey)
    inside, outside = (5, 6), (4, 7)
    for g in inside:
        features_of(g)
    network(inside)
    for g in far:
        middle_weights(g, (0,))
        late_sides(g)
    arrive(far_cols + near_relay)
    for ex in range(1, EX - 1):
        flip(ex, 0)
        flip(ex, EY - 1)
    flip(EX - 1, 0)
    flip(EX - 1, EY - 1)
    for g in outside:
        features_of(g)
    network(outside)
    held = forces_of([unit for g in inside + outside for unit in ghost_units(g)])
    for ey in range(EY):
        ghost_f[EX - 1, ey] = force_tile(EX - 1, ey)
    start(f_copies[5:8])
    settle(held)

    arrive(far_outer + far_relay)
    for ey in (0, 1, 2, 3, 6, 7, 8, 9):
        flip(0, ey)
    for g in (0, 3):
        features_of(g)
    network((0, 3))
    held = forces_of([unit for g in (0, 3) for unit in ghost_units(g)])
    for ey in (0, EY - 1):
        for ex in range(EX - 1):
            ghost_f[ex, ey] = force_tile(ex, ey)
    start(f_copies[1:5])
    settle(held)
    arrive(far_inner)
    for ey in (4, 5):
        flip(0, ey)
    for g in (1, 2):
        features_of(g)
    network((1, 2))
    held = forces_of([unit for g in (1, 2) for unit in ghost_units(g)])
    for ey in range(1, EY - 1):
        ghost_f[0, ey] = force_tile(0, ey)
    start(f_copies[0:1])
    settle(held)
    settle(forces_of([unit for g in near for unit in inner_units(g)]))
    settle(forces_of([unit for g in far for unit in inner_units(g)]))
    for g in range(GROUPS):
        x, y = spot(g)
        for b in range(2):
            turned = jnp.transpose(shares[g, b * ATOMS : (b + 1) * ATOMS])
            energy = jnp.sum(turned, axis=0, keepdims=True)
            out[3 * BX + home(x), y + b : y + b + 1, :] = jnp.where(lane < cnt[home(x), y + b], energy, 0.0)
    for x in range(BX):
        for y in range(BY):
            sums[1 + x, 1 + y, 0:8] = force_tile(1 + x, 1 + y)
    arrive(f_copies)
    for x in range(BX):
        outer = 0 if x == 0 else EX - 1
        for y in range(BY):
            tile = sums[1 + x, 1 + y, 0:8] + recv_f[outer, 1 + y]
            if y == 0:
                tile = tile + recv_f[1 + x, 0] + recv_f[outer, 0]
            if y == BY - 1:
                tile = tile + recv_f[1 + x, EY - 1] + recv_f[outer, EY - 1]
            for c in range(3):
                out[c * BX + home(x), y : y + 1, :] = tile[c : c + 1]
    for copies in (p_copies, e_copies, f_copies):
        for copy in copies:
            copy.wait_send()


def unpack(packed, forces, energies):
    forces[...] = packed[0 : 3 * BX]
    energies[...] = packed[3 * BX :]


def solution(mesh):
    nx, ny = mesh.shape["gx"], mesh.shape["gy"]

    def body(positions, embed, counts, neighbours, w_one, bias_one, w_two, w_out):
        hbm = pl.BlockSpec(memory_space=pl.ANY)
        vmem = pl.BlockSpec(memory_space=pltpu.VMEM)
        packed = pl.pallas_call(
            functools.partial(kernel, nx, ny),
            out_shape=pltpu.VMEM((4 * BX, BY, ATOMS), F32),
            in_specs=[hbm] * 8,
            out_specs=vmem,
            scratch_shapes=[
                pltpu.VMEM((EX, EY, ATOMS, FEAT), BF16),
                pltpu.VMEM((EX, EY, FEAT, ATOMS), BF16),
                pltpu.VMEM((EX, EY, 8, ATOMS), F32),
                pltpu.VMEM((EX, EY, 8, ATOMS), F32),
                pltpu.VMEM((EX, EY, 128, ATOMS), BF16),
                pltpu.VMEM((BX, BY, ATOMS, 128), BF16),
                pltpu.VMEM((GROUPS, 3, 2 * ATOMS, 2 * ATOMS), BF16),
                pltpu.VMEM((GROUPS, 2, ATOMS, 3 * ATOMS), BF16),
                pltpu.VMEM((GROUPS, 2 * ATOMS, FEAT), BF16),
                pltpu.VMEM((GROUPS, 2 * ATOMS, HID), F32),
                pltpu.VMEM((GROUPS, 2 * ATOMS, FEAT), BF16),
                pltpu.VMEM((GROUPS, 2 * ATOMS, 128), F32),
                pltpu.VMEM((EX, EY, 16, ATOMS), F32),
                pltpu.VMEM((EX, EY, 8, ATOMS), F32),
                pltpu.VMEM((EX, EY, 8, ATOMS), F32),
                pltpu.VMEM((3, BX, BY, ATOMS), F32),
                pltpu.SMEM((BX, BY), jnp.int32),
                pltpu.SMEM((BX, BY, 9), jnp.int32),
                pltpu.VMEM((FEAT, HID), BF16),
                pltpu.VMEM((1, HID), F32),
                pltpu.VMEM((HID, HID), BF16),
                pltpu.VMEM((1, HID), F32),
                pltpu.VMEM((HID, FEAT), BF16),
                pltpu.VMEM((HID, HID), BF16),
                pltpu.SemaphoreType.DMA((9,)),
                pltpu.SemaphoreType.DMA((8,)),
                pltpu.SemaphoreType.DMA((8,)),
                pltpu.SemaphoreType.DMA((14,)),
                pltpu.SemaphoreType.DMA((14,)),
                pltpu.SemaphoreType.DMA((8,)),
                pltpu.SemaphoreType.DMA((8,)),
            ],
            compiler_params=pltpu.CompilerParams(
                collective_id=0, has_side_effects=True, vmem_limit_bytes=60 * 1024 * 1024
            ),
        )(positions, embed, counts, neighbours, w_one, bias_one[None], w_two, w_out[None])
        forces, energies = pl.pallas_call(
            unpack,
            out_shape=(
                jax.ShapeDtypeStruct((3 * BX, BY, ATOMS), F32),
                jax.ShapeDtypeStruct((BX, BY, ATOMS), F32),
            ),
            in_specs=[vmem],
            out_specs=(vmem, vmem),
        )(pltpu.with_memory_space_constraint(packed, pltpu.VMEM))
        return forces.reshape(3, BX, BY, ATOMS), energies

    in_specs = (
        P(None, "gx", "gy", None),
        P("gx", "gy", None, None),
        P("gx", "gy"),
        P("gx", "gy", None),
        P(),
        P(),
        P(),
        P(),
    )
    out_specs = (P(None, "gx", "gy", None), P("gx", "gy", None))
    return jax.shard_map(body, mesh=mesh, in_specs=in_specs, out_specs=out_specs, check_vma=False)
```
